32 devices in a mesh: groups: 2 (over x), patch: 16 (over z, y, core).
Axes of the slice: x: 2, y: 2, z: 4, core: 2. Of those that a mesh axis runs over, the one named last changes fastest.
Arguments:
- queries: bfloat16 [1024, 1536], P(('groups', 'patch')), parts along dimension 0, may hold values from -8 to 8
- fresh_keys: bfloat16 [1024, 1536], P(('groups', 'patch')), parts along dimension 0, may hold values from -8 to 8
- fresh_values: bfloat16 [1024, 1536], P(('groups', 'patch')), parts along dimension 0, may hold values from -128 to 128
- stale_keys: bfloat16 [1024, 1536], P(('groups', 'patch')), parts along dimension 0, may hold values from -8 to 8
- stale_values: bfloat16 [1024, 1536], P(('groups', 'patch')), parts along dimension 0, may hold values from -128 to 128
- text_keys: bfloat16 [452, 1536], P('groups'), parts along dimension 0, may hold values from -8 to 8
- text_values: bfloat16 [452, 1536], P('groups'), parts along dimension 0, may hold values from -128 to 128
- out_weight: bfloat16 [1536, 3072], P(None, 'patch'), may hold values from -0.15625 to 0.15625
- gate_table: float32 [50, 3072], replicated, may hold values from 0.1 to 1.9
- timestep: int32 [2], P('groups'), parts along dimension 0, may hold values from 0 to 49
Outputs:
- branch: bfloat16 [1024, 3072], P(('groups', 'patch')), parts along dimension 0
The draws below stay inside these ranges and needn't reach their ends.
There are 2 independent parts, one for each index of `groups`. The reference program is written for one: setup_inputs(seed, part) draws one part's arguments, and reference() takes and returns one part's arrays. A program takes and returns all parts, laid end to end along the dimension named above; an argument that names none is the same for every part. Nothing has to cross between parts.
All inputs are finite; a program needn't handle non-finite values.
Results may differ from the reference program's by a relative error of at most 0.0095.
Values may be sent and summed in bfloat16 or wider, within the bound.
No kernel may reach another device: no remote copies, remote signals or barrier semaphores. Data moves between devices by JAX's collectives and lax.ppermute only.
A program may use at most 128 MiB of HBM per device.

```python
import jax
import jax.numpy as jnp
from jax import lax

D = 3072
HEAD_DIM = 64
TEXT = 226
HEADS = 24
STEPS = 50
TOK_DEV = 32
TOKENS = 512
N_PATCH = 16


def draw_queries(key, part):
    normal_part = jax.random.truncated_normal(jax.random.fold_in(key, 1), -8.0, 8.0, (TOKENS, HEADS * HEAD_DIM), jnp.float32)
    return normal_part.astype(jnp.bfloat16)


def draw_text_keys(key, part):
    normal_part = jax.random.truncated_normal(jax.random.fold_in(key, 2), -8.0, 8.0, (TEXT, HEADS * HEAD_DIM), jnp.float32)
    return normal_part.astype(jnp.bfloat16)


def shard_levels(stream_key, dims, split, least, largest):
    factor_of = 1.0
    for position, blocks in split:
        steps = jax.random.uniform(jax.random.fold_in(jax.random.fold_in(stream_key, 6), position), (blocks,), jnp.float32, least / len(split), largest / len(split))
        factor_of = factor_of * jnp.repeat(jnp.exp(steps), dims[position] // blocks).reshape((-1,) + (1,) * (len(dims) - 1 - position))
    return factor_of


def scatter_about(own_key, extent, deviation, reach, shards=(), kind=jnp.bfloat16):
    values = deviation * jax.random.normal(own_key, extent, jnp.float32)
    if shards:
        values = values * shard_levels(own_key, extent, shards, -0.22, 0.18)
    return jnp.clip(values, -reach, reach).astype(kind)


def setup_inputs(seed: int = 0, part: int = 0) -> dict:
    splits = jax.random.split(jax.random.key(seed), 11)
    part_splits = jax.random.split(jax.random.fold_in(splits[10], part), 11)
    return {
        "queries": draw_queries(jax.random.fold_in(jax.random.fold_in(splits[10], part), 71), part),
        "fresh_keys": scatter_about(part_splits[1], (TOKENS, HEADS * HEAD_DIM), 1.0, 8.0, ((0, 16),)),
        "fresh_values": scatter_about(part_splits[2], (TOKENS, HEADS * HEAD_DIM), 24.0, 128.0, ((0, 16),)),
        "stale_keys": scatter_about(part_splits[3], (TOKENS, HEADS * HEAD_DIM), 1.0, 8.0, ((0, 16),)),
        "stale_values": scatter_about(part_splits[4], (TOKENS, HEADS * HEAD_DIM), 24.0, 128.0, ((0, 16),)),
        "text_keys": draw_text_keys(jax.random.fold_in(jax.random.fold_in(splits[10], part), 71), part),
        "text_values": scatter_about(part_splits[6], (TEXT, HEADS * HEAD_DIM), 24.0, 128.0),
        "out_weight": scatter_about(splits[7], (HEADS * HEAD_DIM, D), (HEADS * HEAD_DIM) ** -0.5, 0.15625, ((1, 16),)),
        "gate_table": jnp.clip(1.0 + 0.18 * jax.random.normal(splits[8], (STEPS, D), jnp.float32), 0.1, 1.9),
        "timestep": jax.random.randint(part_splits[9], (1,), 0, STEPS).astype(jnp.int32),
    }


def reference(queries, fresh_keys, fresh_values, stale_keys, stale_values, text_keys, text_values, out_weight, gate_table, timestep):
    gating = gate_table[timestep[0]]
    scaling = HEAD_DIM ** -0.5

    def one_patch(patch_id):
        offset = (patch_id * TOK_DEV).astype(jnp.int32)
        query = lax.dynamic_slice_in_dim(queries, offset, TOK_DEV, 0).astype(jnp.float32).reshape(TOK_DEV, HEADS, HEAD_DIM)
        key_video = lax.dynamic_update_slice_in_dim(stale_keys, lax.dynamic_slice_in_dim(fresh_keys, offset, TOK_DEV, 0), offset, 0)
        value_video = lax.dynamic_update_slice_in_dim(stale_values, lax.dynamic_slice_in_dim(fresh_values, offset, TOK_DEV, 0), offset, 0)
        key_rows = jnp.concatenate([text_keys, key_video], 0).astype(jnp.float32).reshape(-1, HEADS, HEAD_DIM)
        value_rows = jnp.concatenate([text_values, value_video], 0).astype(jnp.float32).reshape(-1, HEADS, HEAD_DIM)
        scores = jnp.einsum("thd,shd->ths", query, key_rows) * scaling
        highest = jnp.max(scores, -1)
        expo = jnp.exp(scores - highest[..., None])
        total = jnp.sum(expo, -1)
        probs = lax.optimization_barrier(expo.astype(jnp.bfloat16)).astype(jnp.float32)
        weighted = jnp.einsum("ths,shd->thd", probs, value_rows)
        attended = (weighted / total[..., None]).reshape(TOK_DEV, HEADS * HEAD_DIM).astype(jnp.bfloat16)
        projected = jnp.dot(attended, out_weight, preferred_element_type=jnp.float32)
        return (projected * gating[None, :]).astype(jnp.bfloat16)

    blocks = lax.map(one_patch, jnp.arange(N_PATCH, dtype=jnp.int32))
    return blocks.reshape(TOKENS, D)
```

```python
import functools
import math

import jax
import jax.numpy as jnp
from jax import lax
from jax.experimental import pallas as pl
from jax.experimental.pallas import tpu as pltpu
from jax.sharding import PartitionSpec as P

HEAD_DIM = 64
LANES = 128


def from_behind(shard, axis, by):
    peers = lax.axis_size(axis)
    return lax.ppermute(shard, axis, [(i, (i + by) % peers) for i in range(peers)])


def pick_group(stacked, position):
    return lax.dynamic_index_in_dim(stacked, position, 0, keepdims=False)


def by_group(matrix, group_count):
    width = matrix.shape[1] // group_count
    return matrix.reshape(matrix.shape[0], group_count, width).transpose(1, 0, 2)


def swap_block(stacked, group_count, position):
    received = [pick_group(stacked, position)]
    for step_size in range(1, group_count):
        payload = pick_group(stacked, (position + step_size) % group_count)
        arrived = []
        for offset_by in (step_size, step_size - group_count):
            arrived.append(from_behind(payload, "patch", offset_by))
        received.append(jnp.where(position >= step_size, arrived[0], arrived[1]))
    ordered = jnp.stack(received, 0)
    order = (position - jnp.arange(group_count, dtype=jnp.int32)) % group_count
    return jnp.take(ordered, order, axis=0)


def general_body(
    queries,
    fresh_keys,
    fresh_values,
    stale_keys,
    stale_values,
    text_keys,
    text_values,
    out_weight,
    gate_table,
    timestep,
):
    row_count = queries.shape[0]
    head_width = HEAD_DIM
    head_count = queries.shape[1] // head_width
    scaling = head_width ** (-0.5)
    device_count = lax.axis_size("patch")
    group_count = math.gcd(math.gcd(head_count, 8), device_count)
    group_heads = head_count // group_count
    group_width = group_heads * head_width
    position = lax.axis_index("patch") % group_count
    block_first = lax.axis_index("patch") // group_count * group_count
    local_stack = jnp.stack(
        [
            by_group(queries, group_count),
            by_group(fresh_keys, group_count),
            by_group(fresh_values, group_count),
        ],
        1,
    )
    block_stack = swap_block(local_stack, group_count, position)
    block_rows_count = group_count * row_count
    block_query = block_stack[:, 0].reshape(block_rows_count, group_heads, head_width)
    block_keys = block_stack[:, 1].reshape(block_rows_count, group_heads, head_width)
    block_values = block_stack[:, 2].reshape(block_rows_count, group_heads, head_width)
    copies = device_count // group_count
    spread_keys = jnp.tile(by_group(stale_keys, group_count), (copies, 1, 1))
    spread_values = jnp.tile(by_group(stale_values, group_count), (copies, 1, 1))
    every_keys, every_values = (
        lax.all_to_all(spread_keys, "patch", split_axis=0, concat_axis=0, tiled=True),
        lax.all_to_all(spread_values, "patch", split_axis=0, concat_axis=0, tiled=True),
    )
    every_keys = every_keys.reshape(device_count * row_count, group_heads, head_width)
    every_values = every_values.reshape(device_count * row_count, group_heads, head_width)
    text_k = pick_group(by_group(text_keys, group_count), position)
    text_k = text_k.reshape(-1, group_heads, head_width)
    text_v = pick_group(by_group(text_values, group_count), position)
    text_v = text_v.reshape(-1, group_heads, head_width)
    query_patch = jnp.arange(block_rows_count, dtype=jnp.int32) // row_count
    stale_patch = jnp.arange(device_count * row_count, dtype=jnp.int32) // row_count
    stale_mask = stale_patch[None, :] != (block_first + query_patch)[:, None]
    fresh_mask = query_patch[None, :] == query_patch[:, None]

    def scored(key_block):
        return (
            jnp.einsum("qhd,khd->qhk", block_query, key_block, preferred_element_type=jnp.float32)
            * scaling
        )

    text_scores = scored(text_k)
    fresh_scores = jnp.where(fresh_mask[:, None, :], scored(block_keys), -1e30)
    stale_scores = jnp.where(stale_mask[:, None, :], scored(every_keys), -1e30)
    highest = jnp.maximum(
        jnp.maximum(jnp.max(text_scores, -1), jnp.max(fresh_scores, -1)), jnp.max(stale_scores, -1)
    )
    text_expo = jnp.exp(text_scores - highest[..., None])
    fresh_expo = jnp.exp(fresh_scores - highest[..., None])
    stale_expo = jnp.exp(stale_scores - highest[..., None])
    total = jnp.sum(text_expo, -1) + jnp.sum(fresh_expo, -1) + jnp.sum(stale_expo, -1)

    def weigh_block(expo, value_block):
        return jnp.einsum(
            "qhk,khd->qhd",
            expo.astype(jnp.bfloat16),
            value_block,
            preferred_element_type=jnp.float32,
        )

    weighted = (
        weigh_block(text_expo, text_v)
        + weigh_block(fresh_expo, block_values)
        + weigh_block(stale_expo, every_values)
    )
    block_out = (
        (weighted / total[..., None])
        .reshape(group_count, row_count, group_width)
        .astype(jnp.bfloat16)
    )
    home = swap_block(block_out, group_count, position)
    attended = home.transpose(1, 0, 2).reshape(row_count, head_count * head_width)
    projected = jnp.dot(
        attended,
        lax.all_gather(out_weight, "patch", axis=1, tiled=True),
        preferred_element_type=jnp.float32,
    )
    selector = (jnp.arange(gate_table.shape[0], dtype=jnp.int32) == timestep[0]).astype(jnp.float32)
    gating = jnp.dot(selector, gate_table, precision=lax.Precision.HIGHEST)
    return (projected * gating[None, :]).astype(jnp.bfloat16)


QUAD = 4
GRANT = 8 * 2**20


def swap(shard, by):
    peers = lax.axis_size("patch")
    return lax.ppermute(shard, "patch", [(i, i ^ by) for i in range(peers)])


def pack_kernel(line_ref, q_ref, fk_ref, fv_ref, sk_ref, sv_ref, *outs):
    lines = len(outs) // 2
    width = q_ref.shape[1] // lines
    for k in range(lines):
        cols = pl.ds(pl.multiple_of((line_ref[0] ^ k) * width, LANES), width)
        outs[k][:, :width] = sk_ref[:, cols]
        outs[k][:, width:] = sv_ref[:, cols]
        fresh = outs[lines + k]
        fresh[:, :width] = q_ref[:, cols]
        fresh[:, width : 2 * width] = fk_ref[:, cols]
        fresh[:, 2 * width :] = fv_ref[:, cols]


def attend_kernel(rows, line_ref, tk_ref, tv_ref, *refs):
    lines = (len(refs) - 4) // 2
    fresh = refs[:lines]
    own = refs[lines : 2 * lines]
    far = refs[2 * lines : 2 * lines + 3]
    out = refs[-1]
    width = out.shape[1]
    count = rows * lines
    nt = (((1,), (1,)), ((), ()))
    nn = (((1,), (0,)), ((), ()))
    lane = lax.broadcasted_iota(jnp.int32, (1, LANES), 1)
    low = lane < HEAD_DIM
    row_block = (lax.broadcasted_iota(jnp.int32, (2 * count, count), 0) % count) // rows
    col_block = lax.broadcasted_iota(jnp.int32, (2 * count, count), 1) // rows
    same = row_block == col_block
    scaling = HEAD_DIM**-0.5
    f32 = jnp.float32
    for pair in range(width // LANES):
        cols = slice(pair * LANES, (pair + 1) * LANES)
        kcols = slice(width + pair * LANES, width + (pair + 1) * LANES)
        vcols = slice(2 * width + pair * LANES, 2 * width + (pair + 1) * LANES)
        q = jnp.concatenate([fresh[k][:, cols] for k in range(lines)], 0)
        q = (q.astype(f32) * scaling).astype(q.dtype)
        zero = jnp.zeros_like(q)
        q2 = jnp.concatenate([jnp.where(low, q, zero), jnp.where(low, zero, q)], 0)
        fk = jnp.concatenate([fresh[k][:, kcols] for k in range(lines)], 0)
        fv = jnp.concatenate([fresh[k][:, vcols] for k in range(lines)], 0)
        sk = jnp.concatenate([own[k][:, cols] for k in range(lines)], 0)
        sv = jnp.concatenate([own[k][:, kcols] for k in range(lines)], 0)
        s_fresh = lax.dot_general(q2, fk, nt, preferred_element_type=f32)
        s_own = lax.dot_general(q2, sk, nt, preferred_element_type=f32)
        s_near = jnp.where(same, s_fresh, s_own)
        s_far = [
            lax.dot_general(q2, ref[:, cols], nt, preferred_element_type=f32) for ref in far
        ]
        s_text = lax.dot_general(q2, tk_ref[:, cols], nt, preferred_element_type=f32)
        top = jnp.max(s_near, -1, keepdims=True)
        for s in s_far + [s_text]:
            top = jnp.maximum(top, jnp.max(s, -1, keepdims=True))
        e_near = jnp.exp(s_near - top)
        total = jnp.sum(e_near, -1, keepdims=True)
        p_near = e_near.astype(jnp.bfloat16)
        none = jnp.zeros_like(p_near)
        acc = lax.dot_general(jnp.where(same, p_near, none), fv, nn, preferred_element_type=f32)
        acc += lax.dot_general(jnp.where(same, none, p_near), sv, nn, preferred_element_type=f32)
        for s, ref in zip(s_far, far):
            e = jnp.exp(s - top)
            total += jnp.sum(e, -1, keepdims=True)
            acc += lax.dot_general(
                e.astype(jnp.bfloat16), ref[:, kcols], nn, preferred_element_type=f32
            )
        e = jnp.exp(s_text - top)
        total += jnp.sum(e, -1, keepdims=True)
        acc += lax.dot_general(
            e.astype(jnp.bfloat16), tv_ref[:, cols], nn, preferred_element_type=f32
        )
        acc = acc / total
        out[:, cols] = jnp.where(low, acc[:count], acc[count:]).astype(out.dtype)


def project_kernel(rows, where_ref, gate_ref, *refs):
    lines = (len(refs) - QUAD) // 2
    att = refs[:lines]
    weights = refs[lines : lines + QUAD]
    outs = refs[lines + QUAD :]
    width = att[0].shape[1]
    nt = (((1,), (1,)), ((), ()))
    line = where_ref[0]
    odd = (where_ref[1] & 1) == 1
    high = where_ref[1] >= 2
    acc = [None] * QUAD
    for k in range(lines):
        a = jnp.concatenate(
            [att[k][(m ^ k) * rows : ((m ^ k) + 1) * rows, :] for m in range(lines)], 0
        )
        span = pl.ds(pl.multiple_of((line ^ k) * width, LANES), width)
        for j in range(QUAD):
            part = lax.dot_general(a, weights[j][:, span], nt, preferred_element_type=jnp.float32)
            acc[j] = part if acc[j] is None else acc[j] + part
    pairs = []
    for j in (0, 2):
        first = jnp.where(odd, acc[j + 1], acc[j])
        second = jnp.where(odd, acc[j], acc[j + 1])
        pairs.append(jnp.concatenate([first, second], 1))
    lower = jnp.where(high, pairs[1], pairs[0])
    upper = jnp.where(high, pairs[0], pairs[1])
    gate = gate_ref[pl.ds(where_ref[2], 1), :]
    result = (jnp.concatenate([lower, upper], 1) * gate).astype(outs[0].dtype)
    for m in range(lines):
        outs[m][...] = result[m * rows : (m + 1) * rows, :]


def place_kernel(line_ref, *refs):
    parts, out = refs[:-1], refs[-1]
    width = parts[0].shape[1]
    for m, part in enumerate(parts):
        out[:, pl.ds(pl.multiple_of((line_ref[0] ^ m) * width, LANES), width)] = part[...]


def square_body(
    queries,
    fresh_keys,
    fresh_values,
    stale_keys,
    stale_values,
    text_keys,
    text_values,
    out_weight,
    gate_table,
    timestep,
):
    rows, model = queries.shape
    index = lax.axis_index("patch")
    lines = lax.axis_size("patch") // QUAD
    width = model // lines
    out_width = out_weight.shape[1] * QUAD
    line = index // QUAD
    seat = index % QUAD
    bf16 = queries.dtype
    line_arr = line.reshape(1)

    def whole(shape):
        return pl.BlockSpec(shape, lambda i, *_: (0,) * len(shape))

    packed = pl.pallas_call(
        pack_kernel,
        grid_spec=pltpu.PrefetchScalarGridSpec(
            num_scalar_prefetch=1,
            grid=(1,),
            in_specs=[whole((rows, model))] * 5,
            out_specs=[whole((rows, 2 * width))] * lines + [whole((rows, 3 * width))] * lines,
        ),
        out_shape=[jax.ShapeDtypeStruct((rows, 2 * width), bf16)] * lines
        + [jax.ShapeDtypeStruct((rows, 3 * width), bf16)] * lines,
        compiler_params=pltpu.CompilerParams(vmem_limit_bytes=GRANT),
        name="pack",
    )(line_arr, queries, fresh_keys, fresh_values, stale_keys, stale_values)
    stale, fresh = packed[:lines], packed[lines:]
    stale = [stale[0]] + [swap(stale[k], QUAD * k) for k in range(1, lines)]
    fresh = [fresh[0]] + [swap(fresh[k], QUAD * k) for k in range(1, lines)]
    line_stale = jnp.concatenate(stale, 0)
    by_y = swap(line_stale, 2)
    by_core = swap(line_stale, 1)
    by_both = swap(by_y, 1)

    columns = out_weight.T
    late_columns, by_y = lax.optimization_barrier((columns, by_y))
    weight_y = swap(late_columns, 2)
    weight_core = swap(columns, 1)
    weight_both = swap(weight_y, 1)

    text = text_keys.shape[0]
    count = rows * lines
    text_spec = pl.BlockSpec((text, width), lambda i, ref: (0, ref[0]))
    attended = pl.pallas_call(
        functools.partial(attend_kernel, rows),
        grid_spec=pltpu.PrefetchScalarGridSpec(
            num_scalar_prefetch=1,
            grid=(1,),
            in_specs=[text_spec, text_spec]
            + [whole((rows, 3 * width))] * lines
            + [whole((rows, 2 * width))] * lines
            + [whole((count, 2 * width))] * 3,
            out_specs=whole((count, width)),
        ),
        out_shape=jax.ShapeDtypeStruct((count, width), bf16),
        compiler_params=pltpu.CompilerParams(vmem_limit_bytes=2 * GRANT),
        name="attend",
    )(line_arr, text_keys, text_values, *fresh, *stale, by_core, by_y, by_both)

    gathered = [attended] + [swap(attended, QUAD * k) for k in range(1, lines)]
    steps = gate_table.shape[0]
    parts = pl.pallas_call(
        functools.partial(project_kernel, rows),
        grid_spec=pltpu.PrefetchScalarGridSpec(
            num_scalar_prefetch=1,
            grid=(1,),
            in_specs=[pl.BlockSpec((steps, out_width), lambda i, ref: (0, ref[0]))]
            + [whole((count, width))] * lines
            + [whole(columns.shape)] * QUAD,
            out_specs=[whole((rows, out_width))] * lines,
        ),
        out_shape=[jax.ShapeDtypeStruct((rows, out_width), bf16)] * lines,
        compiler_params=pltpu.CompilerParams(vmem_limit_bytes=2 * GRANT),
        name="project",
    )(
        jnp.stack([line, seat, timestep[0]]),
        gate_table,
        *gathered,
        columns,
        weight_core,
        weight_y,
        weight_both,
    )
    parts = [parts[0]] + [swap(parts[m], QUAD * m) for m in range(1, lines)]
    return pl.pallas_call(
        place_kernel,
        grid_spec=pltpu.PrefetchScalarGridSpec(
            num_scalar_prefetch=1,
            grid=(1,),
            in_specs=[whole((rows, out_width))] * lines,
            out_specs=whole((rows, out_width * lines)),
        ),
        out_shape=jax.ShapeDtypeStruct((rows, out_width * lines), bf16),
        compiler_params=pltpu.CompilerParams(vmem_limit_bytes=GRANT),
        name="place",
    )(line_arr, *parts)


def fits_square(mesh):
    patches = mesh.shape["patch"]
    lines = patches // QUAD
    return patches % QUAD == 0 and lines == QUAD


def solution(mesh):
    in_specs = (
        P(("groups", "patch"), None),
        P(("groups", "patch"), None),
        P(("groups", "patch"), None),
        P(("groups", "patch"), None),
        P(("groups", "patch"), None),
        P("groups", None),
        P("groups", None),
        P(None, "patch"),
        P(),
        P("groups"),
    )
    out_specs = P(("groups", "patch"), None)
    square = fits_square(mesh)

    def body(queries, *rest):
        lines = mesh.shape["patch"] // QUAD
        if square and (queries.shape[1] // lines) % LANES == 0 and queries.shape[0] % 16 == 0:
            return square_body(queries, *rest)
        return general_body(queries, *rest)

    return jax.shard_map(body, mesh=mesh, in_specs=in_specs, out_specs=out_specs, check_vma=False)
```

```python
import functools
import math

import jax
import jax.numpy as jnp
from jax import lax
from jax.experimental import pallas as pl
from jax.experimental.pallas import tpu as pltpu
from jax.sharding import PartitionSpec as P


HEAD_DIM = 64
LANES = 128


def from_behind(shard, axis, by):
    peers = lax.axis_size(axis)
    return lax.ppermute(shard, axis, [(i, (i + by) % peers) for i in range(peers)])


def pick_group(stacked, position):
    return lax.dynamic_index_in_dim(stacked, position, 0, keepdims=False)


def by_group(matrix, group_count):
    width = matrix.shape[1] // group_count
    return matrix.reshape(matrix.shape[0], group_count, width).transpose(1, 0, 2)


def swap_block(stacked, group_count, position):
    received = [pick_group(stacked, position)]
    for step_size in range(1, group_count):
        payload = pick_group(stacked, (position + step_size) % group_count)
        arrived = []
        for offset_by in (step_size, step_size - group_count):
            arrived.append(from_behind(payload, "patch", offset_by))
        received.append(jnp.where(position >= step_size, arrived[0], arrived[1]))
    ordered = jnp.stack(received, 0)
    order = (position - jnp.arange(group_count, dtype=jnp.int32)) % group_count
    return jnp.take(ordered, order, axis=0)


def general_body(
    queries,
    fresh_keys,
    fresh_values,
    stale_keys,
    stale_values,
    text_keys,
    text_values,
    out_weight,
    gate_table,
    timestep,
):
    row_count = queries.shape[0]
    head_width = HEAD_DIM
    head_count = queries.shape[1] // head_width
    scaling = head_width ** (-0.5)
    device_count = lax.axis_size("patch")
    group_count = math.gcd(math.gcd(head_count, 8), device_count)
    group_heads = head_count // group_count
    group_width = group_heads * head_width
    position = lax.axis_index("patch") % group_count
    block_first = lax.axis_index("patch") // group_count * group_count
    local_stack = jnp.stack(
        [
            by_group(queries, group_count),
            by_group(fresh_keys, group_count),
            by_group(fresh_values, group_count),
        ],
        1,
    )
    block_stack = swap_block(local_stack, group_count, position)
    block_rows_count = group_count * row_count
    block_query = block_stack[:, 0].reshape(block_rows_count, group_heads, head_width)
    block_keys = block_stack[:, 1].reshape(block_rows_count, group_heads, head_width)
    block_values = block_stack[:, 2].reshape(block_rows_count, group_heads, head_width)
    copies = device_count // group_count
    spread_keys = jnp.tile(by_group(stale_keys, group_count), (copies, 1, 1))
    spread_values = jnp.tile(by_group(stale_values, group_count), (copies, 1, 1))
    every_keys, every_values = (
        lax.all_to_all(spread_keys, "patch", split_axis=0, concat_axis=0, tiled=True),
        lax.all_to_all(spread_values, "patch", split_axis=0, concat_axis=0, tiled=True),
    )
    every_keys = every_keys.reshape(device_count * row_count, group_heads, head_width)
    every_values = every_values.reshape(device_count * row_count, group_heads, head_width)
    text_k = pick_group(by_group(text_keys, group_count), position)
    text_k = text_k.reshape(-1, group_heads, head_width)
    text_v = pick_group(by_group(text_values, group_count), position)
    text_v = text_v.reshape(-1, group_heads, head_width)
    query_patch = jnp.arange(block_rows_count, dtype=jnp.int32) // row_count
    stale_patch = jnp.arange(device_count * row_count, dtype=jnp.int32) // row_count
    stale_mask = stale_patch[None, :] != (block_first + query_patch)[:, None]
    fresh_mask = query_patch[None, :] == query_patch[:, None]

    def scored(key_block):
        return (
            jnp.einsum("qhd,khd->qhk", block_query, key_block, preferred_element_type=jnp.float32)
            * scaling
        )

    text_scores = scored(text_k)
    fresh_scores = jnp.where(fresh_mask[:, None, :], scored(block_keys), -1e30)
    stale_scores = jnp.where(stale_mask[:, None, :], scored(every_keys), -1e30)
    highest = jnp.maximum(
        jnp.maximum(jnp.max(text_scores, -1), jnp.max(fresh_scores, -1)), jnp.max(stale_scores, -1)
    )
    text_expo = jnp.exp(text_scores - highest[..., None])
    fresh_expo = jnp.exp(fresh_scores - highest[..., None])
    stale_expo = jnp.exp(stale_scores - highest[..., None])
    total = jnp.sum(text_expo, -1) + jnp.sum(fresh_expo, -1) + jnp.sum(stale_expo, -1)

    def weigh_block(expo, value_block):
        return jnp.einsum(
            "qhk,khd->qhd",
            expo.astype(jnp.bfloat16),
            value_block,
            preferred_element_type=jnp.float32,
        )

    weighted = (
        weigh_block(text_expo, text_v)
        + weigh_block(fresh_expo, block_values)
        + weigh_block(stale_expo, every_values)
    )
    block_out = (
        (weighted / total[..., None])
        .reshape(group_count, row_count, group_width)
        .astype(jnp.bfloat16)
    )
    home = swap_block(block_out, group_count, position)
    attended = home.transpose(1, 0, 2).reshape(row_count, head_count * head_width)
    projected = jnp.dot(
        attended,
        lax.all_gather(out_weight, "patch", axis=1, tiled=True),
        preferred_element_type=jnp.float32,
    )
    selector = (jnp.arange(gate_table.shape[0], dtype=jnp.int32) == timestep[0]).astype(jnp.float32)
    gating = jnp.dot(selector, gate_table, precision=lax.Precision.HIGHEST)
    return (projected * gating[None, :]).astype(jnp.bfloat16)


QUAD = 4
GRANT = 8 * 2**20


def swap(shard, by):
    peers = lax.axis_size("patch")
    return lax.ppermute(shard, "patch", [(i, i ^ by) for i in range(peers)])


def pack_kernel(q_ref, fk_ref, fv_ref, sk_ref, sv_ref, *refs):
    outs, sem = refs[:-1], refs[-1]
    lines = len(outs) // 2
    line = lax.axis_index("patch") // QUAD
    width = q_ref.shape[1] // lines
    copies = []
    for half, sources in ((0, (sk_ref, sv_ref)), (lines, (q_ref, fk_ref, fv_ref))):
        for k in reversed(range(lines)):
            cols = pl.ds(pl.multiple_of((line ^ k) * width, LANES), width)
            for t, source in enumerate(sources):
                copy = pltpu.make_async_copy(
                    source.at[:, cols],
                    outs[half + k].at[:, t * width : (t + 1) * width],
                    sem.at[len(copies)],
                )
                copy.start()
                copies.append(copy)
    for copy in copies:
        copy.wait()


def fetch_kernel(step_ref, tk_ref, tv_ref, gate_ref, tk_out, tv_out, gate_out, sem):
    width, out_width = tk_out.shape[1], gate_out.shape[1]
    line = lax.axis_index("patch") // QUAD
    cols = pl.ds(pl.multiple_of(line * width, LANES), width)
    gate_cols = pl.ds(pl.multiple_of(line * out_width, LANES), out_width)
    copies = [
        pltpu.make_async_copy(tk_ref.at[:, cols], tk_out, sem.at[0]),
        pltpu.make_async_copy(tv_ref.at[:, cols], tv_out, sem.at[1]),
        pltpu.make_async_copy(gate_ref.at[pl.ds(step_ref[0], 1), gate_cols], gate_out, sem.at[2]),
    ]
    for copy in copies:
        copy.start()
    for copy in copies:
        copy.wait()


def join_kernel(*refs):
    parts, out = refs[:-1], refs[-1]
    rows = parts[0].shape[0]
    for k, part in enumerate(parts):
        out[k * rows : (k + 1) * rows, :] = part[...]


def attend_kernel(rows, tk_ref, tv_ref, *refs):
    lines = (len(refs) - 4) // 2
    fresh = refs[:lines]
    own = refs[lines : 2 * lines]
    far = refs[2 * lines : 2 * lines + 3]
    out = refs[-1]
    width = out.shape[1]
    count = rows * lines
    nt = (((1,), (1,)), ((), ()))
    nn = (((1,), (0,)), ((), ()))
    lane = lax.broadcasted_iota(jnp.int32, (1, LANES), 1)
    low = lane < HEAD_DIM
    row_block = (lax.broadcasted_iota(jnp.int32, (2 * count, count), 0) % count) // rows
    col_block = lax.broadcasted_iota(jnp.int32, (2 * count, count), 1) // rows
    same = row_block == col_block
    scaling = HEAD_DIM**-0.5
    f32 = jnp.float32
    for pair in range(width // LANES):
        cols = slice(pair * LANES, (pair + 1) * LANES)
        kcols = slice(width + pair * LANES, width + (pair + 1) * LANES)
        vcols = slice(2 * width + pair * LANES, 2 * width + (pair + 1) * LANES)
        q = jnp.concatenate([fresh[k][:, cols] for k in range(lines)], 0)
        q = (q.astype(f32) * scaling).astype(q.dtype)
        zero = jnp.zeros_like(q)
        q2 = jnp.concatenate([jnp.where(low, q, zero), jnp.where(low, zero, q)], 0)
        fk = jnp.concatenate([fresh[k][:, kcols] for k in range(lines)], 0)
        fv = jnp.concatenate([fresh[k][:, vcols] for k in range(lines)], 0)
        sk = jnp.concatenate([own[k][:, cols] for k in range(lines)], 0)
        sv = jnp.concatenate([own[k][:, kcols] for k in range(lines)], 0)
        s_fresh = lax.dot_general(q2, fk, nt, preferred_element_type=f32)
        s_own = lax.dot_general(q2, sk, nt, preferred_element_type=f32)
        s_near = jnp.where(same, s_fresh, s_own)
        s_far = [
            lax.dot_general(q2, ref[:, cols], nt, preferred_element_type=f32) for ref in far
        ]
        s_text = lax.dot_general(q2, tk_ref[:, cols], nt, preferred_element_type=f32)
        top = jnp.max(s_near, -1, keepdims=True)
        for s in s_far + [s_text]:
            top = jnp.maximum(top, jnp.max(s, -1, keepdims=True))
        e_near = jnp.exp(s_near - top)
        total = jnp.sum(e_near, -1, keepdims=True)
        p_near = e_near.astype(jnp.bfloat16)
        none = jnp.zeros_like(p_near)
        acc = lax.dot_general(jnp.where(same, p_near, none), fv, nn, preferred_element_type=f32)
        acc += lax.dot_general(jnp.where(same, none, p_near), sv, nn, preferred_element_type=f32)
        for s, ref in zip(s_far, far):
            e = jnp.exp(s - top)
            total += jnp.sum(e, -1, keepdims=True)
            acc += lax.dot_general(
                e.astype(jnp.bfloat16), ref[:, kcols], nn, preferred_element_type=f32
            )
        e = jnp.exp(s_text - top)
        total += jnp.sum(e, -1, keepdims=True)
        acc += lax.dot_general(
            e.astype(jnp.bfloat16), tv_ref[:, cols], nn, preferred_element_type=f32
        )
        acc = acc / total
        out[:, cols] = jnp.where(low, acc[:count], acc[count:]).astype(out.dtype)


def project_kernel(rows, gate_ref, *refs):
    lines = (len(refs) - QUAD) // 2
    att = refs[:lines]
    weights = refs[lines : lines + QUAD]
    outs = refs[lines + QUAD :]
    width = att[0].shape[1]
    nt = (((1,), (1,)), ((), ()))
    index = lax.axis_index("patch")
    line = index // QUAD
    odd = (index & 1) == 1
    high = (index & 2) == 2
    acc = [None] * QUAD
    for k in range(lines):
        a = jnp.concatenate(
            [att[k][(m ^ k) * rows : ((m ^ k) + 1) * rows, :] for m in range(lines)], 0
        )
        span = pl.ds(pl.multiple_of((line ^ k) * width, LANES), width)
        for j in range(QUAD):
            part = lax.dot_general(a, weights[j][:, span], nt, preferred_element_type=jnp.float32)
            acc[j] = part if acc[j] is None else acc[j] + part
    pairs = []
    for j in (0, 2):
        first = jnp.where(odd, acc[j + 1], acc[j])
        second = jnp.where(odd, acc[j], acc[j + 1])
        pairs.append(jnp.concatenate([first, second], 1))
    lower = jnp.where(high, pairs[1], pairs[0])
    upper = jnp.where(high, pairs[0], pairs[1])
    result = (jnp.concatenate([lower, upper], 1) * gate_ref[...]).astype(outs[0].dtype)
    for m in range(lines):
        outs[m][...] = result[m * rows : (m + 1) * rows, :]


def place_kernel(*refs):
    line = lax.axis_index("patch") // QUAD
    parts, out = refs[:-1], refs[-1]
    width = parts[0].shape[1]
    for m, part in enumerate(parts):
        out[:, pl.ds(pl.multiple_of((line ^ m) * width, LANES), width)] = part[...]


def square_body(
    queries,
    fresh_keys,
    fresh_values,
    stale_keys,
    stale_values,
    text_keys,
    text_values,
    out_weight,
    gate_table,
    timestep,
):
    rows, model = queries.shape
    lines = lax.axis_size("patch") // QUAD
    width = model // lines
    out_width = out_weight.shape[1] * QUAD
    count = rows * lines
    text = text_keys.shape[0]
    bf16 = queries.dtype
    vmem = pl.BlockSpec(memory_space=pltpu.VMEM)
    hbm = pl.BlockSpec(memory_space=pltpu.HBM)
    smem = pl.BlockSpec(memory_space=pltpu.SMEM)

    def shaped(*shape, dtype=bf16):
        return jax.ShapeDtypeStruct(shape, dtype)

    def in_hbm(*arrays):
        return [pltpu.with_memory_space_constraint(array, pltpu.HBM) for array in arrays]

    def kernel(body, outs, specs, scratch=(), grant=1):
        return pl.pallas_call(
            body,
            in_specs=specs,
            out_specs=jax.tree.map(lambda _: vmem, outs),
            out_shape=outs,
            scratch_shapes=scratch,
            compiler_params=pltpu.CompilerParams(vmem_limit_bytes=grant * GRANT),
        )

    others = list(reversed(range(1, lines)))
    packed = kernel(
        pack_kernel,
        [shaped(rows, 2 * width)] * lines + [shaped(rows, 3 * width)] * lines,
        [hbm] * 5,
        [pltpu.SemaphoreType.DMA((5 * lines,))],
    )(*in_hbm(queries, fresh_keys, fresh_values, stale_keys, stale_values))
    stale, fresh = list(packed[:lines]), list(packed[lines:])
    for k in others:
        stale[k] = swap(stale[k], QUAD * k)
    for k in others:
        fresh[k] = swap(fresh[k], QUAD * k)
    text_k, text_v, gate = kernel(
        fetch_kernel,
        [shaped(text, width), shaped(text, width), shaped(1, out_width, dtype=jnp.float32)],
        [smem, hbm, hbm, hbm],
        [pltpu.SemaphoreType.DMA((3,))],
    )(timestep, *in_hbm(text_keys, text_values, gate_table))
    line_stale = kernel(join_kernel, shaped(count, 2 * width), [vmem] * lines)(*stale)
    by_y = swap(line_stale, 2)
    by_core = swap(line_stale, 1)
    by_both = swap(by_y, 1)

    columns = out_weight.T
    late_columns, by_y = lax.optimization_barrier((columns, by_y))
    weight_y = swap(late_columns, 2)
    weight_core = swap(columns, 1)
    weight_both = swap(weight_y, 1)

    attended = kernel(
        functools.partial(attend_kernel, rows),
        shaped(count, width),
        [vmem] * (2 * lines + 5),
        grant=2,
    )(text_k, text_v, *fresh, *stale, by_core, by_y, by_both)

    gathered = [attended] * lines
    for k in others:
        gathered[k] = swap(attended, QUAD * k)
    parts = kernel(
        functools.partial(project_kernel, rows),
        [shaped(rows, out_width)] * lines,
        [vmem] * (1 + lines + QUAD),
        grant=2,
    )(gate, *gathered, columns, weight_core, weight_y, weight_both)
    parts = list(parts)
    for k in others:
        parts[k] = swap(parts[k], QUAD * k)
    return kernel(place_kernel, shaped(rows, out_width * lines), [vmem] * lines)(*parts)


def solution(mesh):
    in_specs = (
        P(("groups", "patch"), None),
        P(("groups", "patch"), None),
        P(("groups", "patch"), None),
        P(("groups", "patch"), None),
        P(("groups", "patch"), None),
        P("groups", None),
        P("groups", None),
        P(None, "patch"),
        P(),
        P("groups"),
    )
    out_specs = P(("groups", "patch"), None)
    lines = mesh.shape["patch"] // QUAD

    square = mesh.shape["patch"] == QUAD * lines and lines == QUAD

    def body(queries, *rest):
        if square and (queries.shape[1] // lines) % LANES == 0 and queries.shape[0] % 16 == 0:
            return square_body(queries, *rest)
        return general_body(queries, *rest)

    return jax.shard_map(body, mesh=mesh, in_specs=in_specs, out_specs=out_specs, check_vma=False)
```

```python
import functools
import math

import jax
import jax.numpy as jnp
from jax import lax
from jax.experimental import pallas as pl
from jax.experimental.pallas import tpu as pltpu
from jax.sharding import PartitionSpec as P


HEAD_DIM = 64
LANES = 128


def from_behind(shard, axis, by):
    peers = lax.axis_size(axis)
    return lax.ppermute(shard, axis, [(i, (i + by) % peers) for i in range(peers)])


def pick_group(stacked, position):
    return lax.dynamic_index_in_dim(stacked, position, 0, keepdims=False)


def by_group(matrix, group_count):
    width = matrix.shape[1] // group_count
    return matrix.reshape(matrix.shape[0], group_count, width).transpose(1, 0, 2)


def swap_block(stacked, group_count, position):
    received = [pick_group(stacked, position)]
    for step_size in range(1, group_count):
        payload = pick_group(stacked, (position + step_size) % group_count)
        arrived = []
        for offset_by in (step_size, step_size - group_count):
            arrived.append(from_behind(payload, "patch", offset_by))
        received.append(jnp.where(position >= step_size, arrived[0], arrived[1]))
    ordered = jnp.stack(received, 0)
    order = (position - jnp.arange(group_count, dtype=jnp.int32)) % group_count
    return jnp.take(ordered, order, axis=0)


def general_body(
    queries,
    fresh_keys,
    fresh_values,
    stale_keys,
    stale_values,
    text_keys,
    text_values,
    out_weight,
    gate_table,
    timestep,
):
    row_count = queries.shape[0]
    head_width = HEAD_DIM
    head_count = queries.shape[1] // head_width
    scaling = head_width ** (-0.5)
    device_count = lax.axis_size("patch")
    group_count = math.gcd(math.gcd(head_count, 8), device_count)
    group_heads = head_count // group_count
    group_width = group_heads * head_width
    position = lax.axis_index("patch") % group_count
    block_first = lax.axis_index("patch") // group_count * group_count
    local_stack = jnp.stack(
        [
            by_group(queries, group_count),
            by_group(fresh_keys, group_count),
            by_group(fresh_values, group_count),
        ],
        1,
    )
    block_stack = swap_block(local_stack, group_count, position)
    block_rows_count = group_count * row_count
    block_query = block_stack[:, 0].reshape(block_rows_count, group_heads, head_width)
    block_keys = block_stack[:, 1].reshape(block_rows_count, group_heads, head_width)
    block_values = block_stack[:, 2].reshape(block_rows_count, group_heads, head_width)
    copies = device_count // group_count
    spread_keys = jnp.tile(by_group(stale_keys, group_count), (copies, 1, 1))
    spread_values = jnp.tile(by_group(stale_values, group_count), (copies, 1, 1))
    every_keys, every_values = (
        lax.all_to_all(spread_keys, "patch", split_axis=0, concat_axis=0, tiled=True),
        lax.all_to_all(spread_values, "patch", split_axis=0, concat_axis=0, tiled=True),
    )
    every_keys = every_keys.reshape(device_count * row_count, group_heads, head_width)
    every_values = every_values.reshape(device_count * row_count, group_heads, head_width)
    text_k = pick_group(by_group(text_keys, group_count), position)
    text_k = text_k.reshape(-1, group_heads, head_width)
    text_v = pick_group(by_group(text_values, group_count), position)
    text_v = text_v.reshape(-1, group_heads, head_width)
    query_patch = jnp.arange(block_rows_count, dtype=jnp.int32) // row_count
    stale_patch = jnp.arange(device_count * row_count, dtype=jnp.int32) // row_count
    stale_mask = stale_patch[None, :] != (block_first + query_patch)[:, None]
    fresh_mask = query_patch[None, :] == query_patch[:, None]

    def scored(key_block):
        return (
            jnp.einsum("qhd,khd->qhk", block_query, key_block, preferred_element_type=jnp.float32)
            * scaling
        )

    text_scores = scored(text_k)
    fresh_scores = jnp.where(fresh_mask[:, None, :], scored(block_keys), -1e30)
    stale_scores = jnp.where(stale_mask[:, None, :], scored(every_keys), -1e30)
    highest = jnp.maximum(
        jnp.maximum(jnp.max(text_scores, -1), jnp.max(fresh_scores, -1)), jnp.max(stale_scores, -1)
    )
    text_expo = jnp.exp(text_scores - highest[..., None])
    fresh_expo = jnp.exp(fresh_scores - highest[..., None])
    stale_expo = jnp.exp(stale_scores - highest[..., None])
    total = jnp.sum(text_expo, -1) + jnp.sum(fresh_expo, -1) + jnp.sum(stale_expo, -1)

    def weigh_block(expo, value_block):
        return jnp.einsum(
            "qhk,khd->qhd",
            expo.astype(jnp.bfloat16),
            value_block,
            preferred_element_type=jnp.float32,
        )

    weighted = (
        weigh_block(text_expo, text_v)
        + weigh_block(fresh_expo, block_values)
        + weigh_block(stale_expo, every_values)
    )
    block_out = (
        (weighted / total[..., None])
        .reshape(group_count, row_count, group_width)
        .astype(jnp.bfloat16)
    )
    home = swap_block(block_out, group_count, position)
    attended = home.transpose(1, 0, 2).reshape(row_count, head_count * head_width)
    projected = jnp.dot(
        attended,
        lax.all_gather(out_weight, "patch", axis=1, tiled=True),
        preferred_element_type=jnp.float32,
    )
    selector = (jnp.arange(gate_table.shape[0], dtype=jnp.int32) == timestep[0]).astype(jnp.float32)
    gating = jnp.dot(selector, gate_table, precision=lax.Precision.HIGHEST)
    return (projected * gating[None, :]).astype(jnp.bfloat16)


QUAD = 4
GRANT = 8 * 2**20


def swap(shard, by):
    peers = lax.axis_size("patch")
    return lax.ppermute(shard, "patch", [(i, i ^ by) for i in range(peers)])


def line_slices(refs, outs, line):
    width = refs[0].shape[1] // len(outs)
    copies = []
    for k in reversed(range(len(outs))):
        cols = pl.ds(pl.multiple_of((line ^ k) * width, LANES), width)
        for t, ref in enumerate(refs):
            copies.append((ref.at[:, cols], outs[k].at[:, t * width : (t + 1) * width]))
    return copies


def pack_kernel(q_ref, fk_ref, fv_ref, sk_ref, sv_ref, w_ref, *refs):
    outs, w_out, sem = refs[:-2], refs[-2], refs[-1]
    lines = len(outs) // 2
    line = lax.axis_index("patch") // QUAD
    copies = line_slices((sk_ref, sv_ref), outs[:lines], line)
    copies += line_slices((q_ref, fk_ref, fv_ref), outs[lines:], line)
    copies.append((w_ref.at[: w_out.shape[0], :], w_out))
    run_copies(copies, sem)


def run_copies(pairs, sem):
    copies = [pltpu.make_async_copy(*pair, sem.at[i]) for i, pair in enumerate(pairs)]
    for copy in copies:
        copy.start()
    for copy in copies:
        copy.wait()


def fetch_kernel(step_ref, tk_ref, tv_ref, gate_ref, w_ref, tk_out, tv_out, gate_out, w_out, sem):
    width, out_width = tk_out.shape[1], gate_out.shape[1]
    line = lax.axis_index("patch") // QUAD
    cols = pl.ds(pl.multiple_of(line * width, LANES), width)
    gate_cols = pl.ds(pl.multiple_of(line * out_width, LANES), out_width)
    copies = [
        (tk_ref.at[:, cols], tk_out),
        (tv_ref.at[:, cols], tv_out),
        (gate_ref.at[pl.ds(step_ref[0], 1), gate_cols], gate_out),
        (w_ref.at[w_ref.shape[0] - w_out.shape[0] :, :], w_out),
    ]
    run_copies(copies, sem)


def join_kernel(*refs):
    parts, out = refs[:-1], refs[-1]
    rows = parts[0].shape[0]
    for k, part in enumerate(parts):
        out[k * rows : (k + 1) * rows, :] = part[...]


NT = (((1,), (1,)), ((), ()))
NN = (((1,), (0,)), ((), ()))


def dot(a, b, dims):
    return lax.dot_general(a, b, dims, preferred_element_type=jnp.float32)


def head_rows(q):
    low = lax.broadcasted_iota(jnp.int32, (1, LANES), 1) < HEAD_DIM
    q = (q.astype(jnp.float32) * HEAD_DIM**-0.5).astype(q.dtype)
    zero = jnp.zeros_like(q)
    return jnp.concatenate([jnp.where(low, q, zero), jnp.where(low, zero, q)], 0)


def early_kernel(tk_ref, tv_ref, *refs):
    lines = (len(refs) - 5) // 2
    fresh, own, core = refs[:lines], refs[lines : 2 * lines], refs[2 * lines]
    q_out, acc_out, top_out, sum_out = refs[2 * lines + 1 :]
    rows, width = fresh[0].shape[0], tk_ref.shape[1]
    count = rows * lines
    row_block = (lax.broadcasted_iota(jnp.int32, (2 * count, count), 0) % count) // rows
    col_block = lax.broadcasted_iota(jnp.int32, (2 * count, count), 1) // rows
    same = row_block == col_block
    for pair in range(width // LANES):
        first = pair * LANES
        cols, kcols, vcols = (
            slice(t * width + first, t * width + first + LANES) for t in range(3)
        )
        q = head_rows(jnp.concatenate([ref[:, cols] for ref in fresh], 0))
        fresh_k = jnp.concatenate([ref[:, kcols] for ref in fresh], 0)
        fresh_v = jnp.concatenate([ref[:, vcols] for ref in fresh], 0)
        own_k = jnp.concatenate([ref[:, cols] for ref in own], 0)
        own_v = jnp.concatenate([ref[:, kcols] for ref in own], 0)
        s_near = jnp.where(same, dot(q, fresh_k, NT), dot(q, own_k, NT))
        s_core = dot(q, core[:, cols], NT)
        s_text = dot(q, tk_ref[:, cols], NT)
        top = jnp.maximum(
            jnp.max(jnp.maximum(s_near, s_core), -1, keepdims=True),
            jnp.max(s_text, -1, keepdims=True),
        )
        e_near, e_core, e_text = (jnp.exp(s - top) for s in (s_near, s_core, s_text))
        total = jnp.sum(e_near + e_core, -1, keepdims=True) + jnp.sum(e_text, -1, keepdims=True)
        p_near = e_near.astype(jnp.bfloat16)
        none = jnp.zeros_like(p_near)
        acc = dot(jnp.where(same, p_near, none), fresh_v, NN)
        acc += dot(jnp.where(same, none, p_near), own_v, NN)
        acc += dot(e_core.astype(jnp.bfloat16), core[:, kcols], NN)
        acc += dot(e_text.astype(jnp.bfloat16), tv_ref[:, cols], NN)
        span = slice(2 * count * pair, 2 * count * (pair + 1))
        q_out[span, :] = q
        acc_out[span, :] = acc
        top_out[span, :] = jnp.broadcast_to(top, acc.shape)
        sum_out[span, :] = jnp.broadcast_to(total, acc.shape)


def attend_kernel(q_ref, acc_ref, top_ref, sum_ref, y_ref, both_ref, out):
    count, width = out.shape
    low = lax.broadcasted_iota(jnp.int32, (1, LANES), 1) < HEAD_DIM
    for pair in range(width // LANES):
        cols = slice(pair * LANES, (pair + 1) * LANES)
        vcols = slice(width + pair * LANES, width + (pair + 1) * LANES)
        span = slice(2 * count * pair, 2 * count * (pair + 1))
        keys = jnp.concatenate([y_ref[:, cols], both_ref[:, cols]], 0)
        values = jnp.concatenate([y_ref[:, vcols], both_ref[:, vcols]], 0)
        s = dot(q_ref[span, :], keys, NT)
        top = jnp.maximum(top_ref[span, :], jnp.max(s, -1, keepdims=True))
        shrink = jnp.exp(top_ref[span, :] - top)
        e = jnp.exp(s - jnp.concatenate([top] * (s.shape[1] // LANES), 1))
        total = sum_ref[span, :] * shrink + jnp.sum(e, -1, keepdims=True)
        acc = acc_ref[span, :] * shrink + dot(e.astype(jnp.bfloat16), values, NN)
        acc = acc / total
        out[:, cols] = jnp.where(low, acc[:count], acc[count:]).astype(out.dtype)


def project_kernel(ks, last, *refs):
    weights = refs[: QUAD + 2]
    weights = [weights[:1], weights[1:2], weights[2:4], weights[4:6]]
    att, refs = refs[QUAD + 2 : QUAD + 2 + len(ks)], refs[QUAD + 2 + len(ks) :]
    index = lax.axis_index("patch")
    line = index // QUAD
    width = att[0].shape[1]
    rows = att[0].shape[0] // QUAD
    before = refs[0] if last else None
    acc = [before[j] if last else None for j in range(QUAD)]
    for k, ref in zip(ks, att):
        a = jnp.concatenate([ref[(m ^ k) * rows : ((m ^ k) + 1) * rows, :] for m in range(QUAD)], 0)
        span = pl.ds(pl.multiple_of((line ^ k) * width, LANES), width)
        for j in range(QUAD):
            weight = jnp.concatenate([part[:, span] for part in weights[j]], 0)
            part = dot(a, weight, NT)
            acc[j] = part if acc[j] is None else acc[j] + part
    if not last:
        for j in range(QUAD):
            refs[0][j] = acc[j]
        return
    gate_ref, outs = refs[1], refs[2:]
    odd = (index & 1) == 1
    high = (index & 2) == 2
    pairs = []
    for j in (0, 2):
        near = jnp.where(odd, acc[j + 1], acc[j])
        far = jnp.where(odd, acc[j], acc[j + 1])
        pairs.append(jnp.concatenate([near, far], 1))
    lower = jnp.where(high, pairs[1], pairs[0])
    upper = jnp.where(high, pairs[0], pairs[1])
    result = (jnp.concatenate([lower, upper], 1) * gate_ref[...]).astype(outs[0].dtype)
    for m, out in enumerate(outs):
        out[...] = result[m * rows : (m + 1) * rows, :]


def place_kernel(*refs):
    parts, out, sem = refs[:-2], refs[-2], refs[-1]
    line = lax.axis_index("patch") // QUAD
    width = parts[0].shape[1]
    copies = []
    for m, part in enumerate(parts):
        cols = pl.ds(pl.multiple_of((line ^ m) * width, LANES), width)
        copies.append((part, out.at[:, cols]))
    run_copies(copies, sem)


def square_body(
    queries,
    fresh_keys,
    fresh_values,
    stale_keys,
    stale_values,
    text_keys,
    text_values,
    out_weight,
    gate_table,
    timestep,
):
    rows, model = queries.shape
    lines = lax.axis_size("patch") // QUAD
    width = model // lines
    out_width = out_weight.shape[1] * QUAD
    count = rows * lines
    text = text_keys.shape[0]
    bf16 = queries.dtype
    vmem = pl.BlockSpec(memory_space=pltpu.VMEM)
    hbm = pl.BlockSpec(memory_space=pltpu.HBM)
    smem = pl.BlockSpec(memory_space=pltpu.SMEM)

    def shaped(*shape, dtype=bf16):
        return jax.ShapeDtypeStruct(shape, dtype)

    def in_hbm(*arrays):
        return [pltpu.with_memory_space_constraint(array, pltpu.HBM) for array in arrays]

    def kernel(body, outs, specs, scratch=(), grant=1):
        return pl.pallas_call(
            body,
            in_specs=specs,
            out_specs=jax.tree.map(lambda _: vmem, outs),
            out_shape=outs,
            scratch_shapes=scratch,
            compiler_params=pltpu.CompilerParams(vmem_limit_bytes=grant * GRANT),
        )

    columns = out_weight.T
    half = columns.shape[0] // 2
    others = list(reversed(range(1, lines)))
    *packed, early = kernel(
        pack_kernel,
        [shaped(rows, 2 * width)] * lines
        + [shaped(rows, 3 * width)] * lines
        + [shaped(half, model)],
        [hbm] * 6,
        [pltpu.SemaphoreType.DMA((5 * lines + 1,))],
    )(*in_hbm(queries, fresh_keys, fresh_values, stale_keys, stale_values, columns))
    stale, fresh = packed[:lines], packed[lines:]
    for k in others:
        stale[k] = swap(stale[k], QUAD * k)
    for k in others:
        fresh[k] = swap(fresh[k], QUAD * k)
    text_k, text_v, gate, late = kernel(
        fetch_kernel,
        [shaped(text, width)] * 2
        + [shaped(1, out_width, dtype=jnp.float32), shaped(half, model)],
        [smem] + [hbm] * 4,
        [pltpu.SemaphoreType.DMA((4,))],
    )(timestep, *in_hbm(text_keys, text_values, gate_table, columns))
    line_stale = kernel(join_kernel, shaped(count, 2 * width), [vmem] * lines)(*stale)
    by_y = swap(line_stale, 2)
    by_core = swap(line_stale, 1)
    by_both = swap(by_y, 1)

    weight_y = [swap(early, 2), swap(late, 2)]
    weight_core = swap(columns, 1)
    weight_both = [swap(weight_y[0], 1), swap(weight_y[1], 1)]

    stacked = 2 * count * (width // LANES)
    early_part = kernel(
        early_kernel,
        [shaped(stacked, LANES)] + [shaped(stacked, LANES, dtype=jnp.float32)] * 3,
        [vmem] * (2 * lines + 3),
    )(text_k, text_v, *fresh, *stale, by_core)
    attended = kernel(attend_kernel, shaped(count, width), [vmem] * 6)(*early_part, by_y, by_both)

    gathered = [attended] * lines
    for k in others:
        gathered[k] = swap(attended, QUAD * k)
    weights = [columns, weight_core, *weight_y, *weight_both]
    near_lines, far_lines = tuple(range(lines // 2)), tuple(range(lines // 2, lines))
    sums = kernel(
        functools.partial(project_kernel, near_lines, False),
        shaped(QUAD, count, out_weight.shape[1], dtype=jnp.float32),
        [vmem] * (QUAD + 2 + len(near_lines)),
        grant=2,
    )(*weights, *[gathered[k] for k in near_lines])
    parts = kernel(
        functools.partial(project_kernel, far_lines, True),
        [shaped(rows, out_width)] * lines,
        [vmem] * (QUAD + 4 + len(far_lines)),
        grant=2,
    )(*weights, *[gathered[k] for k in far_lines], sums, gate)
    parts = list(parts)
    for k in others:
        parts[k] = swap(parts[k], QUAD * k)
    return pl.pallas_call(
        place_kernel,
        in_specs=[vmem] * lines,
        out_specs=hbm,
        out_shape=shaped(rows, out_width * lines),
        scratch_shapes=[pltpu.SemaphoreType.DMA((lines,))],
        compiler_params=pltpu.CompilerParams(vmem_limit_bytes=GRANT),
        name="place",
    )(*parts)


def solution(mesh):
    in_specs = (
        P(("groups", "patch"), None),
        P(("groups", "patch"), None),
        P(("groups", "patch"), None),
        P(("groups", "patch"), None),
        P(("groups", "patch"), None),
        P("groups", None),
        P("groups", None),
        P(None, "patch"),
        P(),
        P("groups"),
    )
    out_specs = P(("groups", "patch"), None)
    lines = mesh.shape["patch"] // QUAD

    square = mesh.shape["patch"] == QUAD * lines and lines == QUAD

    def body(queries, *rest):
        if square and (queries.shape[1] // lines) % LANES == 0 and queries.shape[0] % 16 == 0:
            return square_body(queries, *rest)
        return general_body(queries, *rest)

    return jax.shard_map(body, mesh=mesh, in_specs=in_specs, out_specs=out_specs, check_vma=False)
```

```python
import functools
import math

import jax
import jax.numpy as jnp
from jax import lax
from jax.experimental import pallas as pl
from jax.experimental.pallas import tpu as pltpu
from jax.sharding import PartitionSpec as P


HEAD_DIM = 64
LANES = 128


def from_behind(shard, axis, by):
    peers = lax.axis_size(axis)
    return lax.ppermute(shard, axis, [(i, (i + by) % peers) for i in range(peers)])


def pick_group(stacked, position):
    return lax.dynamic_index_in_dim(stacked, position, 0, keepdims=False)


def by_group(matrix, group_count):
    width = matrix.shape[1] // group_count
    return matrix.reshape(matrix.shape[0], group_count, width).transpose(1, 0, 2)


def swap_block(stacked, group_count, position):
    received = [pick_group(stacked, position)]
    for step_size in range(1, group_count):
        payload = pick_group(stacked, (position + step_size) % group_count)
        arrived = []
        for offset_by in (step_size, step_size - group_count):
            arrived.append(from_behind(payload, "patch", offset_by))
        received.append(jnp.where(position >= step_size, arrived[0], arrived[1]))
    ordered = jnp.stack(received, 0)
    order = (position - jnp.arange(group_count, dtype=jnp.int32)) % group_count
    return jnp.take(ordered, order, axis=0)


def general_body(
    queries,
    fresh_keys,
    fresh_values,
    stale_keys,
    stale_values,
    text_keys,
    text_values,
    out_weight,
    gate_table,
    timestep,
):
    row_count = queries.shape[0]
    head_width = HEAD_DIM
    head_count = queries.shape[1] // head_width
    scaling = head_width ** (-0.5)
    device_count = lax.axis_size("patch")
    group_count = math.gcd(math.gcd(head_count, 8), device_count)
    group_heads = head_count // group_count
    group_width = group_heads * head_width
    position = lax.axis_index("patch") % group_count
    block_first = lax.axis_index("patch") // group_count * group_count
    local_stack = jnp.stack(
        [
            by_group(queries, group_count),
            by_group(fresh_keys, group_count),
            by_group(fresh_values, group_count),
        ],
        1,
    )
    block_stack = swap_block(local_stack, group_count, position)
    block_rows_count = group_count * row_count
    block_query = block_stack[:, 0].reshape(block_rows_count, group_heads, head_width)
    block_keys = block_stack[:, 1].reshape(block_rows_count, group_heads, head_width)
    block_values = block_stack[:, 2].reshape(block_rows_count, group_heads, head_width)
    copies = device_count // group_count
    spread_keys = jnp.tile(by_group(stale_keys, group_count), (copies, 1, 1))
    spread_values = jnp.tile(by_group(stale_values, group_count), (copies, 1, 1))
    every_keys, every_values = (
        lax.all_to_all(spread_keys, "patch", split_axis=0, concat_axis=0, tiled=True),
        lax.all_to_all(spread_values, "patch", split_axis=0, concat_axis=0, tiled=True),
    )
    every_keys = every_keys.reshape(device_count * row_count, group_heads, head_width)
    every_values = every_values.reshape(device_count * row_count, group_heads, head_width)
    text_k = pick_group(by_group(text_keys, group_count), position)
    text_k = text_k.reshape(-1, group_heads, head_width)
    text_v = pick_group(by_group(text_values, group_count), position)
    text_v = text_v.reshape(-1, group_heads, head_width)
    query_patch = jnp.arange(block_rows_count, dtype=jnp.int32) // row_count
    stale_patch = jnp.arange(device_count * row_count, dtype=jnp.int32) // row_count
    stale_mask = stale_patch[None, :] != (block_first + query_patch)[:, None]
    fresh_mask = query_patch[None, :] == query_patch[:, None]

    def scored(key_block):
        return (
            jnp.einsum("qhd,khd->qhk", block_query, key_block, preferred_element_type=jnp.float32)
            * scaling
        )

    text_scores = scored(text_k)
    fresh_scores = jnp.where(fresh_mask[:, None, :], scored(block_keys), -1e30)
    stale_scores = jnp.where(stale_mask[:, None, :], scored(every_keys), -1e30)
    highest = jnp.maximum(
        jnp.maximum(jnp.max(text_scores, -1), jnp.max(fresh_scores, -1)), jnp.max(stale_scores, -1)
    )
    text_expo = jnp.exp(text_scores - highest[..., None])
    fresh_expo = jnp.exp(fresh_scores - highest[..., None])
    stale_expo = jnp.exp(stale_scores - highest[..., None])
    total = jnp.sum(text_expo, -1) + jnp.sum(fresh_expo, -1) + jnp.sum(stale_expo, -1)

    def weigh_block(expo, value_block):
        return jnp.einsum(
            "qhk,khd->qhd",
            expo.astype(jnp.bfloat16),
            value_block,
            preferred_element_type=jnp.float32,
        )

    weighted = (
        weigh_block(text_expo, text_v)
        + weigh_block(fresh_expo, block_values)
        + weigh_block(stale_expo, every_values)
    )
    block_out = (
        (weighted / total[..., None])
        .reshape(group_count, row_count, group_width)
        .astype(jnp.bfloat16)
    )
    home = swap_block(block_out, group_count, position)
    attended = home.transpose(1, 0, 2).reshape(row_count, head_count * head_width)
    projected = jnp.dot(
        attended,
        lax.all_gather(out_weight, "patch", axis=1, tiled=True),
        preferred_element_type=jnp.float32,
    )
    selector = (jnp.arange(gate_table.shape[0], dtype=jnp.int32) == timestep[0]).astype(jnp.float32)
    gating = jnp.dot(selector, gate_table, precision=lax.Precision.HIGHEST)
    return (projected * gating[None, :]).astype(jnp.bfloat16)


QUAD = 4
GRANT = 8 * 2**20


def swap(shard, by):
    peers = lax.axis_size("patch")
    return lax.ppermute(shard, "patch", [(i, i ^ by) for i in range(peers)])


def line_slices(refs, outs, line):
    width = refs[0].shape[1] // len(outs)
    copies = []
    for k in reversed(range(len(outs))):
        cols = pl.ds(pl.multiple_of((line ^ k) * width, LANES), width)
        for t, ref in enumerate(refs):
            copies.append((ref.at[:, cols], outs[k].at[:, t * width : (t + 1) * width]))
    return copies


def pack_kernel(q_ref, fk_ref, fv_ref, sk_ref, sv_ref, w_ref, *refs):
    outs, w_out, sem = refs[:-2], refs[-2], refs[-1]
    lines = len(outs) // 2
    line = lax.axis_index("patch") // QUAD
    copies = line_slices((sk_ref, sv_ref), outs[:lines], line)
    copies += line_slices((q_ref, fk_ref, fv_ref), outs[lines:], line)
    copies.append((w_ref.at[: w_out.shape[0], :], w_out))
    run_copies(copies, sem)


def run_copies(pairs, sem):
    copies = [pltpu.make_async_copy(*pair, sem.at[i]) for i, pair in enumerate(pairs)]
    for copy in copies:
        copy.start()
    for copy in copies:
        copy.wait()


def fetch_kernel(step_ref, tk_ref, tv_ref, gate_ref, w_ref, tk_out, tv_out, gate_out, w_out, sem):
    width, out_width = tk_out.shape[1], gate_out.shape[1]
    line = lax.axis_index("patch") // QUAD
    cols = pl.ds(pl.multiple_of(line * width, LANES), width)
    gate_cols = pl.ds(pl.multiple_of(line * out_width, LANES), out_width)
    copies = [
        (tk_ref.at[:, cols], tk_out),
        (tv_ref.at[:, cols], tv_out),
        (gate_ref.at[pl.ds(step_ref[0], 1), gate_cols], gate_out),
        (w_ref.at[w_ref.shape[0] - w_out.shape[0] :, :], w_out),
    ]
    run_copies(copies, sem)


def join_kernel(*refs):
    parts, out = refs[:-1], refs[-1]
    rows = parts[0].shape[0]
    for k, part in enumerate(parts):
        out[k * rows : (k + 1) * rows, :] = part[...]


NT = (((1,), (1,)), ((), ()))
NN = (((1,), (0,)), ((), ()))


def dot(a, b, dims):
    return lax.dot_general(a, b, dims, preferred_element_type=jnp.float32)


def head_rows(q):
    low = lax.broadcasted_iota(jnp.int32, (1, LANES), 1) < HEAD_DIM
    q = (q.astype(jnp.float32) * HEAD_DIM**-0.5).astype(q.dtype)
    zero = jnp.zeros_like(q)
    return jnp.concatenate([jnp.where(low, q, zero), jnp.where(low, zero, q)], 0)


def early_kernel(tk_ref, tv_ref, *refs):
    lines = (len(refs) - 5) // 2
    fresh, own, core = refs[:lines], refs[lines : 2 * lines], refs[2 * lines]
    q_out, acc_out, top_out, sum_out = refs[2 * lines + 1 :]
    rows, width = fresh[0].shape[0], tk_ref.shape[1]
    count = rows * lines
    row_block = (lax.broadcasted_iota(jnp.int32, (2 * count, count), 0) % count) // rows
    col_block = lax.broadcasted_iota(jnp.int32, (2 * count, count), 1) // rows
    same = row_block == col_block
    for pair in range(width // LANES):
        first = pair * LANES
        cols, kcols, vcols = (
            slice(t * width + first, t * width + first + LANES) for t in range(3)
        )
        q = head_rows(jnp.concatenate([ref[:, cols] for ref in fresh], 0))
        fresh_k = jnp.concatenate([ref[:, kcols] for ref in fresh], 0)
        fresh_v = jnp.concatenate([ref[:, vcols] for ref in fresh], 0)
        own_k = jnp.concatenate([ref[:, cols] for ref in own], 0)
        own_v = jnp.concatenate([ref[:, kcols] for ref in own], 0)
        s_near = jnp.where(same, dot(q, fresh_k, NT), dot(q, own_k, NT))
        s_core = dot(q, core[:, cols], NT)
        s_text = dot(q, tk_ref[:, cols], NT)
        top = jnp.maximum(
            jnp.max(jnp.maximum(s_near, s_core), -1, keepdims=True),
            jnp.max(s_text, -1, keepdims=True),
        )
        e_near, e_core, e_text = (jnp.exp(s - top) for s in (s_near, s_core, s_text))
        total = jnp.sum(e_near + e_core, -1, keepdims=True) + jnp.sum(e_text, -1, keepdims=True)
        p_near = e_near.astype(jnp.bfloat16)
        none = jnp.zeros_like(p_near)
        acc = dot(jnp.where(same, p_near, none), fresh_v, NN)
        acc += dot(jnp.where(same, none, p_near), own_v, NN)
        acc += dot(e_core.astype(jnp.bfloat16), core[:, kcols], NN)
        acc += dot(e_text.astype(jnp.bfloat16), tv_ref[:, cols], NN)
        span = slice(2 * count * pair, 2 * count * (pair + 1))
        q_out[span, :] = q
        acc_out[span, :] = acc
        top_out[span, :] = jnp.broadcast_to(top, acc.shape)
        sum_out[span, :] = jnp.broadcast_to(total, acc.shape)


def attend_kernel(q_ref, acc_ref, top_ref, sum_ref, y_ref, both_ref, *outs):
    count, width = outs[0].shape
    lines = (len(outs) + 1) // 2
    rows = count // lines
    low = lax.broadcasted_iota(jnp.int32, (1, LANES), 1) < HEAD_DIM
    for pair in range(width // LANES):
        cols = slice(pair * LANES, (pair + 1) * LANES)
        vcols = slice(width + pair * LANES, width + (pair + 1) * LANES)
        span = slice(2 * count * pair, 2 * count * (pair + 1))
        keys = jnp.concatenate([y_ref[:, cols], both_ref[:, cols]], 0)
        values = jnp.concatenate([y_ref[:, vcols], both_ref[:, vcols]], 0)
        s = dot(q_ref[span, :], keys, NT)
        top = jnp.maximum(top_ref[span, :], jnp.max(s, -1, keepdims=True))
        shrink = jnp.exp(top_ref[span, :] - top)
        e = jnp.exp(s - jnp.concatenate([top] * (s.shape[1] // LANES), 1))
        total = sum_ref[span, :] * shrink + jnp.sum(e, -1, keepdims=True)
        acc = acc_ref[span, :] * shrink + dot(e.astype(jnp.bfloat16), values, NN)
        acc = acc / total
        both = jnp.where(low, acc[:count], acc[count:]).astype(outs[0].dtype)
        outs[0][:, cols] = both
        for k in range(1, lines):
            outs[k][: k * rows, cols] = both[: k * rows]
            if k < lines - 1:
                outs[k][k * rows :, cols] = both[(k + 1) * rows :]
            outs[lines + k - 1][:, cols] = both[k * rows : (k + 1) * rows]


def project_kernel(ks, own_rows, first, last, *refs):
    weights, refs = refs[: QUAD + 2], refs[QUAD + 2 :]
    weights = [weights[:1], weights[1:2], weights[2:4], weights[4:6]]
    att, refs = refs[: len(ks)], refs[len(ks) :]
    index = lax.axis_index("patch")
    line = index // QUAD
    acc = [None] * QUAD
    if not first:
        acc, refs = [refs[0][j] for j in range(QUAD)], refs[1:]
    width = att[0].shape[1]

    def block(ref, i, rows):
        return ref[i * rows : (i + 1) * rows, :]

    for k, ref in zip(ks, att):
        if own_rows:
            a = block(ref, 0, ref.shape[0] // QUAD) if k == 0 else ref[...]
        elif k == 0:
            a = ref[ref.shape[0] // QUAD :, :]
        else:
            spots = [(m ^ k) - ((m ^ k) > k) for m in range(1, QUAD)]
            a = jnp.concatenate([block(ref, i, ref.shape[0] // len(spots)) for i in spots], 0)
        span = pl.ds(pl.multiple_of((line ^ k) * width, LANES), width)
        for j in range(QUAD):
            weight = jnp.concatenate([part[:, span] for part in weights[j]], 0)
            part = dot(a, weight, NT)
            acc[j] = part if acc[j] is None else acc[j] + part
    if not last:
        for j in range(QUAD):
            refs[0][j] = acc[j]
        return
    gate_ref, outs = refs[0], refs[1:]
    odd = (index & 1) == 1
    high = (index & 2) == 2
    pairs = []
    for j in (0, 2):
        near = jnp.where(odd, acc[j + 1], acc[j])
        far = jnp.where(odd, acc[j], acc[j + 1])
        pairs.append(jnp.concatenate([near, far], 1))
    lower = jnp.where(high, pairs[1], pairs[0])
    upper = jnp.where(high, pairs[0], pairs[1])
    result = (jnp.concatenate([lower, upper], 1) * gate_ref[...]).astype(outs[0].dtype)
    for m, out in enumerate(outs):
        out[...] = block(result, m, out.shape[0])


def place_kernel(*refs):
    parts, out, sem = refs[:-2], refs[-2], refs[-1]
    line = lax.axis_index("patch") // QUAD
    width = parts[0].shape[1]
    copies = []
    for m, part in enumerate(parts):
        cols = pl.ds(pl.multiple_of((line ^ m) * width, LANES), width)
        copies.append((part, out.at[:, cols]))
    run_copies(copies, sem)


def square_body(
    queries,
    fresh_keys,
    fresh_values,
    stale_keys,
    stale_values,
    text_keys,
    text_values,
    out_weight,
    gate_table,
    timestep,
):
    rows, model = queries.shape
    lines = lax.axis_size("patch") // QUAD
    width = model // lines
    out_width = out_weight.shape[1] * QUAD
    count = rows * lines
    text = text_keys.shape[0]
    bf16 = queries.dtype
    vmem = pl.BlockSpec(memory_space=pltpu.VMEM)
    hbm = pl.BlockSpec(memory_space=pltpu.HBM)
    smem = pl.BlockSpec(memory_space=pltpu.SMEM)

    def shaped(*shape, dtype=bf16):
        return jax.ShapeDtypeStruct(shape, dtype)

    def in_hbm(*arrays):
        return [pltpu.with_memory_space_constraint(array, pltpu.HBM) for array in arrays]

    def kernel(body, outs, specs, scratch=(), grant=1):
        return pl.pallas_call(
            body,
            in_specs=specs,
            out_specs=jax.tree.map(lambda _: vmem, outs),
            out_shape=outs,
            scratch_shapes=scratch,
            compiler_params=pltpu.CompilerParams(vmem_limit_bytes=grant * GRANT),
        )

    columns = out_weight.T
    half = columns.shape[0] // 2
    others = list(reversed(range(1, lines)))
    *packed, early = kernel(
        pack_kernel,
        [shaped(rows, 2 * width)] * lines
        + [shaped(rows, 3 * width)] * lines
        + [shaped(half, model)],
        [hbm] * 6,
        [pltpu.SemaphoreType.DMA((5 * lines + 1,))],
    )(*in_hbm(queries, fresh_keys, fresh_values, stale_keys, stale_values, columns))
    stale, fresh = packed[:lines], packed[lines:]
    for k in others:
        stale[k] = swap(stale[k], QUAD * k)
    for k in others:
        fresh[k] = swap(fresh[k], QUAD * k)
    text_k, text_v, gate, late = kernel(
        fetch_kernel,
        [shaped(text, width)] * 2
        + [shaped(1, out_width, dtype=jnp.float32), shaped(half, model)],
        [smem] + [hbm] * 4,
        [pltpu.SemaphoreType.DMA((4,))],
    )(timestep, *in_hbm(text_keys, text_values, gate_table, columns))
    line_stale = kernel(join_kernel, shaped(count, 2 * width), [vmem] * lines)(*stale)
    by_y = swap(line_stale, 2)
    by_core = swap(line_stale, 1)
    by_both = swap(by_y, 1)

    weight_y = [swap(early, 2), swap(late, 2)]
    weight_core = swap(columns, 1)
    weight_both = [swap(weight_y[0], 1), swap(weight_y[1], 1)]

    stacked = 2 * count * (width // LANES)
    early_part = kernel(
        early_kernel,
        [shaped(stacked, LANES)] + [shaped(stacked, LANES, dtype=jnp.float32)] * 3,
        [vmem] * (2 * lines + 3),
    )(text_k, text_v, *fresh, *stale, by_core)
    attended, *blocks = kernel(
        attend_kernel,
        [shaped(count, width)]
        + [shaped(count - rows, width)] * (lines - 1)
        + [shaped(rows, width)] * (lines - 1),
        [vmem] * 6,
    )(*early_part, by_y, by_both)
    theirs, mine = [attended, *blocks[: lines - 1]], [attended, *blocks[lines - 1 :]]
    for k in others:
        theirs[k] = swap(theirs[k], QUAD * k)
    for k in others:
        mine[k] = swap(mine[k], QUAD * k)
    weights = [columns, weight_core, *weight_y, *weight_both]

    def project(ks, own_rows, attended, before, outs):
        first, last = before is None, isinstance(outs, list)
        more = ([] if first else [before]) + ([gate] if last else [])
        return kernel(
            functools.partial(project_kernel, ks, own_rows, first, last),
            outs,
            [vmem] * (len(weights) + len(ks) + len(more)),
            grant=2,
        )(*weights, *[attended[k] for k in ks], *more)

    near, far, every = (0, 1), tuple(range(2, lines)), tuple(range(lines))
    sums = shaped(QUAD, count - rows, out_weight.shape[1], dtype=jnp.float32)
    made = shaped(rows, out_width)
    sums = project(near, False, theirs, None, sums)
    parts = [None, *project(far, False, theirs, sums, [made] * (lines - 1))]
    for k in others:
        parts[k] = swap(parts[k], QUAD * k)
    parts[0] = project(every, True, mine, None, [made])[0]
    return pl.pallas_call(
        place_kernel,
        in_specs=[vmem] * lines,
        out_specs=hbm,
        out_shape=shaped(rows, out_width * lines),
        scratch_shapes=[pltpu.SemaphoreType.DMA((lines,))],
        compiler_params=pltpu.CompilerParams(vmem_limit_bytes=GRANT),
        name="place",
    )(*parts)


def solution(mesh):
    in_specs = (
        P(("groups", "patch"), None),
        P(("groups", "patch"), None),
        P(("groups", "patch"), None),
        P(("groups", "patch"), None),
        P(("groups", "patch"), None),
        P("groups", None),
        P("groups", None),
        P(None, "patch"),
        P(),
        P("groups"),
    )
    out_specs = P(("groups", "patch"), None)
    lines = mesh.shape["patch"] // QUAD

    square = mesh.shape["patch"] == QUAD * lines and lines == QUAD

    def body(queries, *rest):
        if square and (queries.shape[1] // lines) % LANES == 0 and queries.shape[0] % 16 == 0:
            return square_body(queries, *rest)
        return general_body(queries, *rest)

    return jax.shard_map(body, mesh=mesh, in_specs=in_specs, out_specs=out_specs, check_vma=False)
```

```python
import functools
import math

import jax
import jax.numpy as jnp
from jax import lax
from jax.experimental import pallas as pl
from jax.experimental.pallas import tpu as pltpu
from jax.sharding import PartitionSpec as P


HEAD_DIM = 64
LANES = 128


def from_behind(shard, axis, by):
    peers = lax.axis_size(axis)
    return lax.ppermute(shard, axis, [(i, (i + by) % peers) for i in range(peers)])


def pick_group(stacked, position):
    return lax.dynamic_index_in_dim(stacked, position, 0, keepdims=False)


def by_group(matrix, group_count):
    width = matrix.shape[1] // group_count
    return matrix.reshape(matrix.shape[0], group_count, width).transpose(1, 0, 2)


def swap_block(stacked, group_count, position):
    received = [pick_group(stacked, position)]
    for step_size in range(1, group_count):
        payload = pick_group(stacked, (position + step_size) % group_count)
        arrived = []
        for offset_by in (step_size, step_size - group_count):
            arrived.append(from_behind(payload, "patch", offset_by))
        received.append(jnp.where(position >= step_size, arrived[0], arrived[1]))
    ordered = jnp.stack(received, 0)
    order = (position - jnp.arange(group_count, dtype=jnp.int32)) % group_count
    return jnp.take(ordered, order, axis=0)


def general_body(
    queries,
    fresh_keys,
    fresh_values,
    stale_keys,
    stale_values,
    text_keys,
    text_values,
    out_weight,
    gate_table,
    timestep,
):
    row_count = queries.shape[0]
    head_width = HEAD_DIM
    head_count = queries.shape[1] // head_width
    scaling = head_width ** (-0.5)
    device_count = lax.axis_size("patch")
    group_count = math.gcd(math.gcd(head_count, 8), device_count)
    group_heads = head_count // group_count
    group_width = group_heads * head_width
    position = lax.axis_index("patch") % group_count
    block_first = lax.axis_index("patch") // group_count * group_count
    local_stack = jnp.stack(
        [
            by_group(queries, group_count),
            by_group(fresh_keys, group_count),
            by_group(fresh_values, group_count),
        ],
        1,
    )
    block_stack = swap_block(local_stack, group_count, position)
    block_rows_count = group_count * row_count
    block_query = block_stack[:, 0].reshape(block_rows_count, group_heads, head_width)
    block_keys = block_stack[:, 1].reshape(block_rows_count, group_heads, head_width)
    block_values = block_stack[:, 2].reshape(block_rows_count, group_heads, head_width)
    copies = device_count // group_count
    spread_keys = jnp.tile(by_group(stale_keys, group_count), (copies, 1, 1))
    spread_values = jnp.tile(by_group(stale_values, group_count), (copies, 1, 1))
    every_keys, every_values = (
        lax.all_to_all(spread_keys, "patch", split_axis=0, concat_axis=0, tiled=True),
        lax.all_to_all(spread_values, "patch", split_axis=0, concat_axis=0, tiled=True),
    )
    every_keys = every_keys.reshape(device_count * row_count, group_heads, head_width)
    every_values = every_values.reshape(device_count * row_count, group_heads, head_width)
    text_k = pick_group(by_group(text_keys, group_count), position)
    text_k = text_k.reshape(-1, group_heads, head_width)
    text_v = pick_group(by_group(text_values, group_count), position)
    text_v = text_v.reshape(-1, group_heads, head_width)
    query_patch = jnp.arange(block_rows_count, dtype=jnp.int32) // row_count
    stale_patch = jnp.arange(device_count * row_count, dtype=jnp.int32) // row_count
    stale_mask = stale_patch[None, :] != (block_first + query_patch)[:, None]
    fresh_mask = query_patch[None, :] == query_patch[:, None]

    def scored(key_block):
        return (
            jnp.einsum("qhd,khd->qhk", block_query, key_block, preferred_element_type=jnp.float32)
            * scaling
        )

    text_scores = scored(text_k)
    fresh_scores = jnp.where(fresh_mask[:, None, :], scored(block_keys), -1e30)
    stale_scores = jnp.where(stale_mask[:, None, :], scored(every_keys), -1e30)
    highest = jnp.maximum(
        jnp.maximum(jnp.max(text_scores, -1), jnp.max(fresh_scores, -1)), jnp.max(stale_scores, -1)
    )
    text_expo = jnp.exp(text_scores - highest[..., None])
    fresh_expo = jnp.exp(fresh_scores - highest[..., None])
    stale_expo = jnp.exp(stale_scores - highest[..., None])
    total = jnp.sum(text_expo, -1) + jnp.sum(fresh_expo, -1) + jnp.sum(stale_expo, -1)

    def weigh_block(expo, value_block):
        return jnp.einsum(
            "qhk,khd->qhd",
            expo.astype(jnp.bfloat16),
            value_block,
            preferred_element_type=jnp.float32,
        )

    weighted = (
        weigh_block(text_expo, text_v)
        + weigh_block(fresh_expo, block_values)
        + weigh_block(stale_expo, every_values)
    )
    block_out = (
        (weighted / total[..., None])
        .reshape(group_count, row_count, group_width)
        .astype(jnp.bfloat16)
    )
    home = swap_block(block_out, group_count, position)
    attended = home.transpose(1, 0, 2).reshape(row_count, head_count * head_width)
    projected = jnp.dot(
        attended,
        lax.all_gather(out_weight, "patch", axis=1, tiled=True),
        preferred_element_type=jnp.float32,
    )
    selector = (jnp.arange(gate_table.shape[0], dtype=jnp.int32) == timestep[0]).astype(jnp.float32)
    gating = jnp.dot(selector, gate_table, precision=lax.Precision.HIGHEST)
    return (projected * gating[None, :]).astype(jnp.bfloat16)


QUAD = 4
GRANT = 8 * 2**20


def step_to(k):
    return QUAD * k ^ (k in (1, 2))


def swap(shard, by):
    peers = lax.axis_size("patch")
    return lax.ppermute(shard, "patch", [(i, i ^ by) for i in range(peers)])


def line_slices(refs, outs, line):
    width = refs[0].shape[1] // len(outs)
    copies = []
    for k in reversed(range(len(outs))):
        cols = pl.ds(pl.multiple_of((line ^ k) * width, LANES), width)
        for t, ref in enumerate(refs):
            copies.append((ref.at[:, cols], outs[k].at[:, t * width : (t + 1) * width]))
    return copies


def pack_kernel(q_ref, fk_ref, fv_ref, sk_ref, sv_ref, w_ref, *refs):
    outs, w_out, sem = refs[:-2], refs[-2], refs[-1]
    lines = len(outs) // 2
    line = lax.axis_index("patch") // QUAD
    copies = line_slices((sk_ref, sv_ref), outs[:lines], line)
    copies += line_slices((q_ref, fk_ref, fv_ref), outs[lines:], line)
    copies.append((w_ref.at[: w_out.shape[0], :], w_out))
    run_copies(copies, sem)


def run_copies(pairs, sem):
    copies = [pltpu.make_async_copy(*pair, sem.at[i]) for i, pair in enumerate(pairs)]
    for copy in copies:
        copy.start()
    for copy in copies:
        copy.wait()


def fetch_kernel(step_ref, tk_ref, tv_ref, gate_ref, w_ref, tk_out, tv_out, gate_out, w_out, sem):
    width, out_width = tk_out.shape[1], gate_out.shape[1]
    line = lax.axis_index("patch") // QUAD
    cols = pl.ds(pl.multiple_of(line * width, LANES), width)
    gate_cols = pl.ds(pl.multiple_of(line * out_width, LANES), out_width)
    copies = [
        (tk_ref.at[:, cols], tk_out),
        (tv_ref.at[:, cols], tv_out),
        (gate_ref.at[pl.ds(step_ref[0], 1), gate_cols], gate_out),
        (w_ref.at[w_ref.shape[0] - w_out.shape[0] :, :], w_out),
    ]
    run_copies(copies, sem)


def join_kernel(*refs):
    parts, out = refs[:-1], refs[-1]
    rows = parts[0].shape[0]
    for k, part in enumerate(parts):
        out[k * rows : (k + 1) * rows, :] = part[...]


NT = (((1,), (1,)), ((), ()))
NN = (((1,), (0,)), ((), ()))


def dot(a, b, dims):
    return lax.dot_general(a, b, dims, preferred_element_type=jnp.float32)


def head_rows(q):
    low = lax.broadcasted_iota(jnp.int32, (1, LANES), 1) < HEAD_DIM
    q = (q.astype(jnp.float32) * HEAD_DIM**-0.5).astype(q.dtype)
    zero = jnp.zeros_like(q)
    return jnp.concatenate([jnp.where(low, q, zero), jnp.where(low, zero, q)], 0)


def early_kernel(tk_ref, tv_ref, *refs):
    lines = (len(refs) - 5) // 2
    fresh, own, core = refs[:lines], refs[lines : 2 * lines], refs[2 * lines]
    q_out, acc_out, top_out, sum_out = refs[2 * lines + 1 :]
    rows, width = fresh[0].shape[0], tk_ref.shape[1]
    count = rows * lines
    row_block = (lax.broadcasted_iota(jnp.int32, (2 * count, count), 0) % count) // rows
    col_block = lax.broadcasted_iota(jnp.int32, (2 * count, count), 1) // rows
    same = row_block == col_block
    for pair in range(width // LANES):
        first = pair * LANES
        cols, kcols, vcols = (
            slice(t * width + first, t * width + first + LANES) for t in range(3)
        )
        q = head_rows(jnp.concatenate([ref[:, cols] for ref in fresh], 0))
        fresh_k = jnp.concatenate([ref[:, kcols] for ref in fresh], 0)
        fresh_v = jnp.concatenate([ref[:, vcols] for ref in fresh], 0)
        own_k = jnp.concatenate([ref[:, cols] for ref in own], 0)
        own_v = jnp.concatenate([ref[:, kcols] for ref in own], 0)
        s_near = jnp.where(same, dot(q, fresh_k, NT), dot(q, own_k, NT))
        s_core = dot(q, core[:, cols], NT)
        s_text = dot(q, tk_ref[:, cols], NT)
        top = jnp.maximum(
            jnp.max(jnp.maximum(s_near, s_core), -1, keepdims=True),
            jnp.max(s_text, -1, keepdims=True),
        )
        e_near, e_core, e_text = (jnp.exp(s - top) for s in (s_near, s_core, s_text))
        total = jnp.sum(e_near + e_core, -1, keepdims=True) + jnp.sum(e_text, -1, keepdims=True)
        p_near = e_near.astype(jnp.bfloat16)
        none = jnp.zeros_like(p_near)
        acc = dot(jnp.where(same, p_near, none), fresh_v, NN)
        acc += dot(jnp.where(same, none, p_near), own_v, NN)
        acc += dot(e_core.astype(jnp.bfloat16), core[:, kcols], NN)
        acc += dot(e_text.astype(jnp.bfloat16), tv_ref[:, cols], NN)
        span = slice(2 * count * pair, 2 * count * (pair + 1))
        q_out[span, :] = q
        acc_out[span, :] = acc
        top_out[span, :] = jnp.broadcast_to(top, acc.shape)
        sum_out[span, :] = jnp.broadcast_to(total, acc.shape)


def attend_kernel(q_ref, acc_ref, top_ref, sum_ref, y_ref, both_ref, *outs):
    count, width = outs[0].shape
    lines = (len(outs) + 1) // 2
    rows = count // lines
    low = lax.broadcasted_iota(jnp.int32, (1, LANES), 1) < HEAD_DIM
    for pair in range(width // LANES):
        cols = slice(pair * LANES, (pair + 1) * LANES)
        vcols = slice(width + pair * LANES, width + (pair + 1) * LANES)
        span = slice(2 * count * pair, 2 * count * (pair + 1))
        keys = jnp.concatenate([y_ref[:, cols], both_ref[:, cols]], 0)
        values = jnp.concatenate([y_ref[:, vcols], both_ref[:, vcols]], 0)
        s = dot(q_ref[span, :], keys, NT)
        top = jnp.maximum(top_ref[span, :], jnp.max(s, -1, keepdims=True))
        shrink = jnp.exp(top_ref[span, :] - top)
        e = jnp.exp(s - jnp.concatenate([top] * (s.shape[1] // LANES), 1))
        total = sum_ref[span, :] * shrink + jnp.sum(e, -1, keepdims=True)
        acc = acc_ref[span, :] * shrink + dot(e.astype(jnp.bfloat16), values, NN)
        acc = acc / total
        both = jnp.where(low, acc[:count], acc[count:]).astype(outs[0].dtype)
        outs[0][:, cols] = both
        for k in range(1, lines):
            outs[k][: k * rows, cols] = both[: k * rows]
            if k < lines - 1:
                outs[k][k * rows :, cols] = both[(k + 1) * rows :]
            outs[lines + k - 1][:, cols] = both[k * rows : (k + 1) * rows]


def project_kernel(ks, own_rows, first, last, *refs):
    weights, refs = refs[: QUAD + 2], refs[QUAD + 2 :]
    weights = [weights[:1], weights[1:2], weights[2:4], weights[4:6]]
    att, refs = refs[: len(ks)], refs[len(ks) :]
    index = lax.axis_index("patch")
    line = index // QUAD
    acc = [None] * QUAD
    if not first:
        acc, refs = [refs[0][j] for j in range(QUAD)], refs[1:]
    width = att[0].shape[1]

    def block(ref, i, rows):
        return ref[i * rows : (i + 1) * rows, :]

    for k, ref in zip(ks, att):
        if own_rows:
            a = block(ref, 0, ref.shape[0] // QUAD) if k == 0 else ref[...]
        elif k == 0:
            a = ref[ref.shape[0] // QUAD :, :]
        else:
            spots = [(m ^ k) - ((m ^ k) > k) for m in range(1, QUAD)]
            a = jnp.concatenate([block(ref, i, ref.shape[0] // len(spots)) for i in spots], 0)
        span = pl.ds(pl.multiple_of((line ^ k) * width, LANES), width)
        for j in range(QUAD):
            weight = jnp.concatenate([part[:, span] for part in weights[j]], 0)
            part = dot(a, weight, NT)
            acc[j] = part if acc[j] is None else acc[j] + part
    if not last:
        for j in range(QUAD):
            refs[0][j] = acc[j]
        return
    gate_ref, outs = refs[0], refs[1:]
    odd = (index & 1) == 1
    high = (index & 2) == 2
    pairs = []
    for j in (0, 2):
        near = jnp.where(odd, acc[j + 1], acc[j])
        far = jnp.where(odd, acc[j], acc[j + 1])
        pairs.append(jnp.concatenate([near, far], 1))
    lower = jnp.where(high, pairs[1], pairs[0])
    upper = jnp.where(high, pairs[0], pairs[1])
    result = (jnp.concatenate([lower, upper], 1) * gate_ref[...]).astype(outs[0].dtype)
    for m, out in enumerate(outs):
        out[...] = block(result, m, out.shape[0])


def place_kernel(*refs):
    parts, out, sem = refs[:-2], refs[-2], refs[-1]
    line = lax.axis_index("patch") // QUAD
    width = parts[0].shape[1]
    copies = []
    for m, part in enumerate(parts):
        cols = pl.ds(pl.multiple_of((line ^ m) * width, LANES), width)
        copies.append((part, out.at[:, cols]))
    run_copies(copies, sem)


def square_body(
    queries,
    fresh_keys,
    fresh_values,
    stale_keys,
    stale_values,
    text_keys,
    text_values,
    out_weight,
    gate_table,
    timestep,
):
    rows, model = queries.shape
    lines = lax.axis_size("patch") // QUAD
    width = model // lines
    out_width = out_weight.shape[1] * QUAD
    count = rows * lines
    text = text_keys.shape[0]
    bf16 = queries.dtype
    vmem = pl.BlockSpec(memory_space=pltpu.VMEM)
    hbm = pl.BlockSpec(memory_space=pltpu.HBM)
    smem = pl.BlockSpec(memory_space=pltpu.SMEM)

    def shaped(*shape, dtype=bf16):
        return jax.ShapeDtypeStruct(shape, dtype)

    def in_hbm(*arrays):
        return [pltpu.with_memory_space_constraint(array, pltpu.HBM) for array in arrays]

    def kernel(body, outs, specs, scratch=(), grant=1):
        return pl.pallas_call(
            body,
            in_specs=specs,
            out_specs=jax.tree.map(lambda _: vmem, outs),
            out_shape=outs,
            scratch_shapes=scratch,
            compiler_params=pltpu.CompilerParams(vmem_limit_bytes=grant * GRANT),
        )

    columns = out_weight.T
    half = columns.shape[0] // 2
    others = list(reversed(range(1, lines)))
    *packed, early = kernel(
        pack_kernel,
        [shaped(rows, 2 * width)] * lines
        + [shaped(rows, 3 * width)] * lines
        + [shaped(half, model)],
        [hbm] * 6,
        [pltpu.SemaphoreType.DMA((5 * lines + 1,))],
    )(*in_hbm(queries, fresh_keys, fresh_values, stale_keys, stale_values, columns))
    stale, fresh = packed[:lines], packed[lines:]
    for k in others:
        stale[k] = swap(stale[k], step_to(k))
    for k in others:
        fresh[k] = swap(fresh[k], step_to(k))
    text_k, text_v, gate, late = kernel(
        fetch_kernel,
        [shaped(text, width)] * 2
        + [shaped(1, out_width, dtype=jnp.float32), shaped(half, model)],
        [smem] + [hbm] * 4,
        [pltpu.SemaphoreType.DMA((4,))],
    )(timestep, *in_hbm(text_keys, text_values, gate_table, columns))
    line_stale = kernel(join_kernel, shaped(count, 2 * width), [vmem] * lines)(*stale)
    by_y = swap(line_stale, 2)
    by_core = swap(line_stale, 1)
    by_both = swap(by_y, 1)

    weight_y = [swap(early, 2), swap(late, 2)]
    weight_core = swap(columns, 1)
    weight_both = [swap(weight_y[0], 1), swap(weight_y[1], 1)]

    stacked = 2 * count * (width // LANES)
    early_part = kernel(
        early_kernel,
        [shaped(stacked, LANES)] + [shaped(stacked, LANES, dtype=jnp.float32)] * 3,
        [vmem] * (2 * lines + 3),
    )(text_k, text_v, *fresh, *stale, by_core)
    attended, *blocks = kernel(
        attend_kernel,
        [shaped(count, width)]
        + [shaped(count - rows, width)] * (lines - 1)
        + [shaped(rows, width)] * (lines - 1),
        [vmem] * 6,
    )(*early_part, by_y, by_both)
    theirs, mine = [attended, *blocks[: lines - 1]], [attended, *blocks[lines - 1 :]]
    for k in others:
        theirs[k] = swap(theirs[k], step_to(k))
    for k in others:
        mine[k] = swap(mine[k], step_to(k))
    weights = [columns, weight_core, *weight_y, *weight_both]

    def project(ks, own_rows, attended, before, outs):
        first, last = before is None, isinstance(outs, list)
        more = ([] if first else [before]) + ([gate] if last else [])
        return kernel(
            functools.partial(project_kernel, ks, own_rows, first, last),
            outs,
            [vmem] * (len(weights) + len(ks) + len(more)),
            grant=2,
        )(*weights, *[attended[k] for k in ks], *more)

    near, far, every = (0, 1), tuple(range(2, lines)), tuple(range(lines))
    sums = shaped(QUAD, count - rows, out_weight.shape[1], dtype=jnp.float32)
    made = shaped(rows, out_width)
    sums = project(near, False, theirs, None, sums)
    parts = [None, *project(far, False, theirs, sums, [made] * (lines - 1))]
    for k in others:
        parts[k] = swap(parts[k], step_to(k))
    parts[0] = project(every, True, mine, None, [made])[0]
    return pl.pallas_call(
        place_kernel,
        in_specs=[vmem] * lines,
        out_specs=hbm,
        out_shape=shaped(rows, out_width * lines),
        scratch_shapes=[pltpu.SemaphoreType.DMA((lines,))],
        compiler_params=pltpu.CompilerParams(vmem_limit_bytes=GRANT),
        name="place",
    )(*parts)


def solution(mesh):
    in_specs = (
        P(("groups", "patch"), None),
        P(("groups", "patch"), None),
        P(("groups", "patch"), None),
        P(("groups", "patch"), None),
        P(("groups", "patch"), None),
        P("groups", None),
        P("groups", None),
        P(None, "patch"),
        P(),
        P("groups"),
    )
    out_specs = P(("groups", "patch"), None)
    lines = mesh.shape["patch"] // QUAD

    square = mesh.shape["patch"] == QUAD * lines and lines == QUAD

    def body(queries, *rest):
        if square and (queries.shape[1] // lines) % LANES == 0 and queries.shape[0] % 16 == 0:
            return square_body(queries, *rest)
        return general_body(queries, *rest)

    return jax.shard_map(body, mesh=mesh, in_specs=in_specs, out_specs=out_specs, check_vma=False)
```

```python
import functools
import math

import jax
import jax.numpy as jnp
from jax import lax
from jax.experimental import pallas as pl
from jax.experimental.pallas import tpu as pltpu
from jax.sharding import PartitionSpec as P


HEAD_DIM = 64
LANES = 128


def from_behind(shard, axis, by):
    peers = lax.axis_size(axis)
    return lax.ppermute(shard, axis, [(i, (i + by) % peers) for i in range(peers)])


def pick_group(stacked, position):
    return lax.dynamic_index_in_dim(stacked, position, 0, keepdims=False)


def by_group(matrix, group_count):
    width = matrix.shape[1] // group_count
    return matrix.reshape(matrix.shape[0], group_count, width).transpose(1, 0, 2)


def swap_block(stacked, group_count, position):
    received = [pick_group(stacked, position)]
    for step_size in range(1, group_count):
        payload = pick_group(stacked, (position + step_size) % group_count)
        arrived = []
        for offset_by in (step_size, step_size - group_count):
            arrived.append(from_behind(payload, "patch", offset_by))
        received.append(jnp.where(position >= step_size, arrived[0], arrived[1]))
    ordered = jnp.stack(received, 0)
    order = (position - jnp.arange(group_count, dtype=jnp.int32)) % group_count
    return jnp.take(ordered, order, axis=0)


def general_body(
    queries,
    fresh_keys,
    fresh_values,
    stale_keys,
    stale_values,
    text_keys,
    text_values,
    out_weight,
    gate_table,
    timestep,
):
    row_count = queries.shape[0]
    head_width = HEAD_DIM
    head_count = queries.shape[1] // head_width
    scaling = head_width ** (-0.5)
    device_count = lax.axis_size("patch")
    group_count = math.gcd(math.gcd(head_count, 8), device_count)
    group_heads = head_count // group_count
    group_width = group_heads * head_width
    position = lax.axis_index("patch") % group_count
    block_first = lax.axis_index("patch") // group_count * group_count
    local_stack = jnp.stack(
        [
            by_group(queries, group_count),
            by_group(fresh_keys, group_count),
            by_group(fresh_values, group_count),
        ],
        1,
    )
    block_stack = swap_block(local_stack, group_count, position)
    block_rows_count = group_count * row_count
    block_query = block_stack[:, 0].reshape(block_rows_count, group_heads, head_width)
    block_keys = block_stack[:, 1].reshape(block_rows_count, group_heads, head_width)
    block_values = block_stack[:, 2].reshape(block_rows_count, group_heads, head_width)
    copies = device_count // group_count
    spread_keys = jnp.tile(by_group(stale_keys, group_count), (copies, 1, 1))
    spread_values = jnp.tile(by_group(stale_values, group_count), (copies, 1, 1))
    every_keys, every_values = (
        lax.all_to_all(spread_keys, "patch", split_axis=0, concat_axis=0, tiled=True),
        lax.all_to_all(spread_values, "patch", split_axis=0, concat_axis=0, tiled=True),
    )
    every_keys = every_keys.reshape(device_count * row_count, group_heads, head_width)
    every_values = every_values.reshape(device_count * row_count, group_heads, head_width)
    text_k = pick_group(by_group(text_keys, group_count), position)
    text_k = text_k.reshape(-1, group_heads, head_width)
    text_v = pick_group(by_group(text_values, group_count), position)
    text_v = text_v.reshape(-1, group_heads, head_width)
    query_patch = jnp.arange(block_rows_count, dtype=jnp.int32) // row_count
    stale_patch = jnp.arange(device_count * row_count, dtype=jnp.int32) // row_count
    stale_mask = stale_patch[None, :] != (block_first + query_patch)[:, None]
    fresh_mask = query_patch[None, :] == query_patch[:, None]

    def scored(key_block):
        return (
            jnp.einsum("qhd,khd->qhk", block_query, key_block, preferred_element_type=jnp.float32)
            * scaling
        )

    text_scores = scored(text_k)
    fresh_scores = jnp.where(fresh_mask[:, None, :], scored(block_keys), -1e30)
    stale_scores = jnp.where(stale_mask[:, None, :], scored(every_keys), -1e30)
    highest = jnp.maximum(
        jnp.maximum(jnp.max(text_scores, -1), jnp.max(fresh_scores, -1)), jnp.max(stale_scores, -1)
    )
    text_expo = jnp.exp(text_scores - highest[..., None])
    fresh_expo = jnp.exp(fresh_scores - highest[..., None])
    stale_expo = jnp.exp(stale_scores - highest[..., None])
    total = jnp.sum(text_expo, -1) + jnp.sum(fresh_expo, -1) + jnp.sum(stale_expo, -1)

    def weigh_block(expo, value_block):
        return jnp.einsum(
            "qhk,khd->qhd",
            expo.astype(jnp.bfloat16),
            value_block,
            preferred_element_type=jnp.float32,
        )

    weighted = (
        weigh_block(text_expo, text_v)
        + weigh_block(fresh_expo, block_values)
        + weigh_block(stale_expo, every_values)
    )
    block_out = (
        (weighted / total[..., None])
        .reshape(group_count, row_count, group_width)
        .astype(jnp.bfloat16)
    )
    home = swap_block(block_out, group_count, position)
    attended = home.transpose(1, 0, 2).reshape(row_count, head_count * head_width)
    projected = jnp.dot(
        attended,
        lax.all_gather(out_weight, "patch", axis=1, tiled=True),
        preferred_element_type=jnp.float32,
    )
    selector = (jnp.arange(gate_table.shape[0], dtype=jnp.int32) == timestep[0]).astype(jnp.float32)
    gating = jnp.dot(selector, gate_table, precision=lax.Precision.HIGHEST)
    return (projected * gating[None, :]).astype(jnp.bfloat16)


QUAD = 4
GRANT = 8 * 2**20


def step_to(k):
    return QUAD * k ^ (k in (1, 2))


def swap(shard, by):
    peers = lax.axis_size("patch")
    return lax.ppermute(shard, "patch", [(i, i ^ by) for i in range(peers)])


def line_slices(refs, outs, line):
    width = refs[0].shape[1] // len(outs)
    copies = []
    for k in reversed(range(len(outs))):
        cols = pl.ds(pl.multiple_of((line ^ k) * width, LANES), width)
        for t, ref in enumerate(refs):
            copies.append((ref.at[:, cols], outs[k].at[:, t * width : (t + 1) * width]))
    return copies


def pack_kernel(q_ref, fk_ref, fv_ref, sk_ref, sv_ref, w_ref, *refs):
    outs, w_out, sem = refs[:-2], refs[-2], refs[-1]
    lines = len(outs) // 2
    line = lax.axis_index("patch") // QUAD
    copies = line_slices((sk_ref, sv_ref), outs[:lines], line)
    copies += line_slices((q_ref, fk_ref, fv_ref), outs[lines:], line)
    copies.append((w_ref.at[: w_out.shape[0], :], w_out))
    run_copies(copies, sem)


def run_copies(pairs, sem):
    copies = [pltpu.make_async_copy(*pair, sem.at[i]) for i, pair in enumerate(pairs)]
    for copy in copies:
        copy.start()
    for copy in copies:
        copy.wait()


def fetch_kernel(step_ref, tk_ref, tv_ref, gate_ref, w_ref, tk_out, tv_out, gate_out, w_out, sem):
    width, out_width = tk_out.shape[1], gate_out.shape[1]
    line = lax.axis_index("patch") // QUAD
    cols = pl.ds(pl.multiple_of(line * width, LANES), width)
    gate_cols = pl.ds(pl.multiple_of(line * out_width, LANES), out_width)
    copies = [
        (tk_ref.at[:, cols], tk_out),
        (tv_ref.at[:, cols], tv_out),
        (gate_ref.at[pl.ds(step_ref[0], 1), gate_cols], gate_out),
        (w_ref.at[w_ref.shape[0] - w_out.shape[0] :, :], w_out),
    ]
    run_copies(copies, sem)


def join_kernel(*refs):
    parts, out = refs[:-1], refs[-1]
    rows = parts[0].shape[0]
    for k, part in enumerate(parts):
        out[k * rows : (k + 1) * rows, :] = part[...]


NT = (((1,), (1,)), ((), ()))
NN = (((1,), (0,)), ((), ()))


def dot(a, b, dims):
    return lax.dot_general(a, b, dims, preferred_element_type=jnp.float32)


def head_rows(q):
    low = lax.broadcasted_iota(jnp.int32, (1, LANES), 1) < HEAD_DIM
    q = (q.astype(jnp.float32) * HEAD_DIM**-0.5).astype(q.dtype)
    zero = jnp.zeros_like(q)
    return jnp.concatenate([jnp.where(low, q, zero), jnp.where(low, zero, q)], 0)


def early_kernel(tk_ref, tv_ref, *refs):
    lines = (len(refs) - 5) // 2
    fresh, own, core = refs[:lines], refs[lines : 2 * lines], refs[2 * lines]
    q_out, acc_out, top_out, sum_out = refs[2 * lines + 1 :]
    rows, width = fresh[0].shape[0], tk_ref.shape[1]
    count = rows * lines
    row_block = (lax.broadcasted_iota(jnp.int32, (2 * count, count), 0) % count) // rows
    col_block = lax.broadcasted_iota(jnp.int32, (2 * count, count), 1) // rows
    same = row_block == col_block
    for pair in range(width // LANES):
        first = pair * LANES
        cols, kcols, vcols = (
            slice(t * width + first, t * width + first + LANES) for t in range(3)
        )
        q = head_rows(jnp.concatenate([ref[:, cols] for ref in fresh], 0))
        fresh_k = jnp.concatenate([ref[:, kcols] for ref in fresh], 0)
        fresh_v = jnp.concatenate([ref[:, vcols] for ref in fresh], 0)
        own_k = jnp.concatenate([ref[:, cols] for ref in own], 0)
        own_v = jnp.concatenate([ref[:, kcols] for ref in own], 0)
        s_near = dot(q, jnp.concatenate([own_k, fresh_k], 0), NT)
        s_near = jnp.where(same, s_near[:, count:], s_near[:, :count])
        s_core = dot(q, core[:, cols], NT)
        s_text = dot(q, tk_ref[:, cols], NT)
        top = jnp.maximum(
            jnp.max(jnp.maximum(s_near, s_core), -1, keepdims=True),
            jnp.max(s_text, -1, keepdims=True),
        )
        e_near, e_core, e_text = (jnp.exp(s - top) for s in (s_near, s_core, s_text))
        total = jnp.sum(e_near + e_core, -1, keepdims=True) + jnp.sum(e_text, -1, keepdims=True)
        p_near = e_near.astype(jnp.bfloat16)
        none = jnp.zeros_like(p_near)
        p_near = jnp.concatenate([jnp.where(same, none, p_near), jnp.where(same, p_near, none)], 1)
        acc = dot(p_near, jnp.concatenate([own_v, fresh_v], 0), NN)
        acc += dot(e_core.astype(jnp.bfloat16), core[:, kcols], NN)
        acc += dot(e_text.astype(jnp.bfloat16), tv_ref[:, cols], NN)
        span = slice(2 * count * pair, 2 * count * (pair + 1))
        q_out[span, :] = q
        acc_out[span, :] = acc
        top_out[span, :] = jnp.broadcast_to(top, acc.shape)
        sum_out[span, :] = jnp.broadcast_to(total, acc.shape)


def attend_kernel(q_ref, acc_ref, top_ref, sum_ref, y_ref, both_ref, *outs):
    count, width = outs[0].shape
    lines = (len(outs) + 1) // 2
    rows = count // lines
    low = lax.broadcasted_iota(jnp.int32, (1, LANES), 1) < HEAD_DIM
    for pair in range(width // LANES):
        cols = slice(pair * LANES, (pair + 1) * LANES)
        vcols = slice(width + pair * LANES, width + (pair + 1) * LANES)
        span = slice(2 * count * pair, 2 * count * (pair + 1))
        keys = jnp.concatenate([y_ref[:, cols], both_ref[:, cols]], 0)
        values = jnp.concatenate([y_ref[:, vcols], both_ref[:, vcols]], 0)
        s = dot(q_ref[span, :], keys, NT)
        top = jnp.maximum(top_ref[span, :], jnp.max(s, -1, keepdims=True))
        shrink = jnp.exp(top_ref[span, :] - top)
        e = jnp.exp(s - jnp.concatenate([top] * (s.shape[1] // LANES), 1))
        total = sum_ref[span, :] * shrink + jnp.sum(e, -1, keepdims=True)
        acc = acc_ref[span, :] * shrink + dot(e.astype(jnp.bfloat16), values, NN)
        acc = jnp.where(low, acc[:count], acc[count:])
        both = (acc / jnp.where(low, total[:count], total[count:])).astype(outs[0].dtype)
        outs[0][:, cols] = both
        for k in range(1, lines):
            outs[k][: k * rows, cols] = both[: k * rows]
            if k < lines - 1:
                outs[k][k * rows :, cols] = both[(k + 1) * rows :]
            outs[lines + k - 1][:, cols] = both[k * rows : (k + 1) * rows]


def project_kernel(ks, own_rows, first, last, *refs):
    weights, refs = refs[: QUAD + 2], refs[QUAD + 2 :]
    att, refs = refs[: len(ks)], refs[len(ks) :]
    index = lax.axis_index("patch")
    line = index // QUAD
    acc = None
    if not first:
        acc, refs = refs[0][...], refs[1:]
    width = att[0].shape[1]

    def block(ref, i, rows):
        return ref[i * rows : (i + 1) * rows, :]

    for k, ref in zip(ks, att):
        if own_rows:
            a = block(ref, 0, ref.shape[0] // QUAD) if k == 0 else ref[...]
        elif k == 0:
            a = ref[ref.shape[0] // QUAD :, :]
        else:
            spots = [(m ^ k) - ((m ^ k) > k) for m in range(1, QUAD)]
            a = jnp.concatenate([block(ref, i, ref.shape[0] // len(spots)) for i in spots], 0)
        span = pl.ds(pl.multiple_of((line ^ k) * width, LANES), width)
        part = dot(a, jnp.concatenate([ref[:, span] for ref in weights], 0), NT)
        acc = part if acc is None else acc + part
    if not last:
        refs[0][...] = acc
        return
    seat_width = weights[0].shape[0]
    acc = [acc[:, j * seat_width : (j + 1) * seat_width] for j in range(QUAD)]
    gate_ref, outs = refs[0], refs[1:]
    odd = (index & 1) == 1
    high = (index & 2) == 2
    pairs = []
    for j in (0, 2):
        near = jnp.where(odd, acc[j + 1], acc[j])
        far = jnp.where(odd, acc[j], acc[j + 1])
        pairs.append(jnp.concatenate([near, far], 1))
    lower = jnp.where(high, pairs[1], pairs[0])
    upper = jnp.where(high, pairs[0], pairs[1])
    result = (jnp.concatenate([lower, upper], 1) * gate_ref[...]).astype(outs[0].dtype)
    for m, out in enumerate(outs):
        out[...] = block(result, m, out.shape[0])


def place_kernel(*refs):
    parts, out, sem = refs[:-2], refs[-2], refs[-1]
    line = lax.axis_index("patch") // QUAD
    width = parts[0].shape[1]
    copies = []
    for m, part in enumerate(parts):
        cols = pl.ds(pl.multiple_of((line ^ m) * width, LANES), width)
        copies.append((part, out.at[:, cols]))
    run_copies(copies, sem)


def square_body(
    queries,
    fresh_keys,
    fresh_values,
    stale_keys,
    stale_values,
    text_keys,
    text_values,
    out_weight,
    gate_table,
    timestep,
):
    rows, model = queries.shape
    lines = lax.axis_size("patch") // QUAD
    width = model // lines
    out_width = out_weight.shape[1] * QUAD
    count = rows * lines
    text = text_keys.shape[0]
    bf16 = queries.dtype
    vmem = pl.BlockSpec(memory_space=pltpu.VMEM)
    hbm = pl.BlockSpec(memory_space=pltpu.HBM)
    smem = pl.BlockSpec(memory_space=pltpu.SMEM)

    def shaped(*shape, dtype=bf16):
        return jax.ShapeDtypeStruct(shape, dtype)

    def in_hbm(*arrays):
        return [pltpu.with_memory_space_constraint(array, pltpu.HBM) for array in arrays]

    def kernel(body, outs, specs, scratch=(), grant=1):
        return pl.pallas_call(
            body,
            in_specs=specs,
            out_specs=jax.tree.map(lambda _: vmem, outs),
            out_shape=outs,
            scratch_shapes=scratch,
            compiler_params=pltpu.CompilerParams(vmem_limit_bytes=grant * GRANT),
        )

    columns = out_weight.T
    half = columns.shape[0] // 2
    others = list(reversed(range(1, lines)))
    *packed, early = kernel(
        pack_kernel,
        [shaped(rows, 2 * width)] * lines
        + [shaped(rows, 3 * width)] * lines
        + [shaped(half, model)],
        [hbm] * 6,
        [pltpu.SemaphoreType.DMA((5 * lines + 1,))],
    )(*in_hbm(queries, fresh_keys, fresh_values, stale_keys, stale_values, columns))
    stale, fresh = packed[:lines], packed[lines:]
    for k in others:
        stale[k] = swap(stale[k], step_to(k))
    for k in others:
        fresh[k] = swap(fresh[k], step_to(k))
    text_k, text_v, gate, late = kernel(
        fetch_kernel,
        [shaped(text, width)] * 2
        + [shaped(1, out_width, dtype=jnp.float32), shaped(half, model)],
        [smem] + [hbm] * 4,
        [pltpu.SemaphoreType.DMA((4,))],
    )(timestep, *in_hbm(text_keys, text_values, gate_table, columns))
    line_stale = kernel(join_kernel, shaped(count, 2 * width), [vmem] * lines)(*stale)
    by_y = swap(line_stale, 2)
    by_core = swap(line_stale, 1)
    by_both = swap(by_y, 1)

    weight_y = [swap(early, 2), swap(late, 2)]
    weight_core = swap(columns, 1)
    weight_both = [swap(weight_y[0], 1), swap(weight_y[1], 1)]

    stacked = 2 * count * (width // LANES)
    early_part = kernel(
        early_kernel,
        [shaped(stacked, LANES)] + [shaped(stacked, LANES, dtype=jnp.float32)] * 3,
        [vmem] * (2 * lines + 3),
    )(text_k, text_v, *fresh, *stale, by_core)
    attended, *blocks = kernel(
        attend_kernel,
        [shaped(count, width)]
        + [shaped(count - rows, width)] * (lines - 1)
        + [shaped(rows, width)] * (lines - 1),
        [vmem] * 6,
    )(*early_part, by_y, by_both)
    theirs, mine = [attended, *blocks[: lines - 1]], [attended, *blocks[lines - 1 :]]
    for k in others:
        theirs[k] = swap(theirs[k], step_to(k))
    for k in others:
        mine[k] = swap(mine[k], step_to(k))
    weights = [columns, weight_core, *weight_y, *weight_both]

    def project(ks, own_rows, attended, before, outs):
        first, last = before is None, isinstance(outs, list)
        more = ([] if first else [before]) + ([gate] if last else [])
        return kernel(
            functools.partial(project_kernel, ks, own_rows, first, last),
            outs,
            [vmem] * (len(weights) + len(ks) + len(more)),
            grant=2,
        )(*weights, *[attended[k] for k in ks], *more)

    near, far, every = (0, 1), tuple(range(2, lines)), tuple(range(lines))
    sums = shaped(count - rows, out_width, dtype=jnp.float32)
    made = shaped(rows, out_width)
    sums = project(near, False, theirs, None, sums)
    parts = [None, *project(far, False, theirs, sums, [made] * (lines - 1))]
    for k in others:
        parts[k] = swap(parts[k], step_to(k))
    parts[0] = project(every, True, mine, None, [made])[0]
    return pl.pallas_call(
        place_kernel,
        in_specs=[vmem] * lines,
        out_specs=hbm,
        out_shape=shaped(rows, out_width * lines),
        scratch_shapes=[pltpu.SemaphoreType.DMA((lines,))],
        compiler_params=pltpu.CompilerParams(vmem_limit_bytes=GRANT),
        name="place",
    )(*parts)


def solution(mesh):
    in_specs = (
        P(("groups", "patch"), None),
        P(("groups", "patch"), None),
        P(("groups", "patch"), None),
        P(("groups", "patch"), None),
        P(("groups", "patch"), None),
        P("groups", None),
        P("groups", None),
        P(None, "patch"),
        P(),
        P("groups"),
    )
    out_specs = P(("groups", "patch"), None)
    lines = mesh.shape["patch"] // QUAD

    square = mesh.shape["patch"] == QUAD * lines and lines == QUAD

    def body(queries, *rest):
        if square and (queries.shape[1] // lines) % LANES == 0 and queries.shape[0] % 16 == 0:
            return square_body(queries, *rest)
        return general_body(queries, *rest)

    return jax.shard_map(body, mesh=mesh, in_specs=in_specs, out_specs=out_specs, check_vma=False)
```
